128 devices in a mesh: dp: 4 (over z), mp: 32 (over y, x, core).
Axes of the slice: x: 4, y: 4, z: 4, core: 2. Of those that a mesh axis runs over, the one named last changes fastest.
Arguments:
- latest_symbol_ids: int32 [256], P('dp'), may hold values from 0 to 65535
- lexicon_table: bfloat16 [65536, 4096], P('dp', 'mp'), may hold values from -40 to 40
- lexicon_layernorm_stretch: bfloat16 [4096], P('mp'), may hold values from 0.29882812 to 3
- lexicon_layernorm_shift: bfloat16 [4096], P('mp'), may hold values from -4 to 4
- recurrent_layernorm_stretch: bfloat16 [4096], P('mp'), may hold values from 0.25 to 1.75
- recurrent_layernorm_shift: bfloat16 [4096], P('mp'), may hold values from -3 to 3
- prior_recurrent_signal: bfloat16 [256, 4096], P('dp', 'mp'), may hold values from -6 to 6
- recurrent_lerp_coefs: bfloat16 [6, 4096], P(None, 'mp'), may hold values from 0 to 1
- forgetting_lowrank_first: bfloat16 [4096, 128], P('mp'), may hold values from -0.09375 to 0.09375
- forgetting_lowrank_second: bfloat16 [128, 4096], P(None, 'mp'), may hold values from -0.5 to 0.5
- forgetting_baseline: bfloat16 [4096], P('mp'), may hold values from -5 to 1
- learning_speed_lowrank_first: bfloat16 [4096, 128], P('mp'), may hold values from -0.09375 to 0.09375
- learning_speed_lowrank_second: bfloat16 [128, 4096], P(None, 'mp'), may hold values from -0.5 to 0.5
- learning_speed_baseline: bfloat16 [4096], P('mp'), may hold values from -2 to 2
- valve_lowrank_first: bfloat16 [4096, 480], P('mp'), may hold values from -0.09375 to 0.09375
- valve_lowrank_second: bfloat16 [480, 4096], P(None, 'mp'), may hold values from -0.25 to 0.25
- erasure_lookup_coefs: bfloat16 [4096], P('mp'), may hold values from 0.5 to 1.5
- lookup_speed_coefs: bfloat16 [4096], P('mp'), may hold values from 0.5 to 1.5
- present_reward_coefs: bfloat16 [4096], P('mp'), may hold values from -4 to 4
- acceptance_projection: bfloat16 [4096, 4096], P(None, 'mp'), may hold values from -0.09375 to 0.09375
- lookup_projection: bfloat16 [4096, 4096], P(None, 'mp'), may hold values from -0.09375 to 0.09375
- payload_projection: bfloat16 [4096, 4096], P(None, 'mp'), may hold values from -0.09375 to 0.09375
- memory_tensor: float32 [256, 64, 64, 64], P('dp', 'mp'), may hold values from -6 to 6
- cluster_layernorm_stretch: bfloat16 [4096], P('mp'), may hold values from 0.25 to 1.75
- cluster_layernorm_shift: bfloat16 [4096], P('mp'), may hold values from -3 to 3
- recurrent_result_proj: bfloat16 [4096, 4096], P('mp'), may hold values from -0.1875 to 0.1875
- feedforward_layernorm_stretch: bfloat16 [4096], P('mp'), may hold values from 0.25 to 1.75
- feedforward_layernorm_shift: bfloat16 [4096], P('mp'), may hold values from -3 to 3
- prior_feedforward_signal: bfloat16 [256, 4096], P('dp', 'mp'), may hold values from -6 to 6
- feedforward_lerp_coefs: bfloat16 [4096], P('mp'), may hold values from 0 to 1
- feedforward_lookup_proj: bfloat16 [4096, 16384], P(None, 'mp'), may hold values from -0.09375 to 0.09375
- feedforward_payload_proj: bfloat16 [16384, 4096], P('mp'), may hold values from -0.09375 to 0.09375
Outputs:
- hidden_out: float32 [256, 4096], P('dp', 'mp')
- refreshed_memory: float32 [256, 64, 64, 64], P('dp', 'mp')
- att_shift: bfloat16 [256, 4096], P('dp', 'mp')
- ffn_shift: bfloat16 [256, 4096], P('dp', 'mp')
- value_first: bfloat16 [256, 4096], P('dp', 'mp')
The draws below stay inside these ranges and needn't reach their ends.
All inputs are finite; a program needn't handle non-finite values.
Results may differ from the reference program's by a relative error of at most 0.0095.
Values may be sent and summed in bfloat16 or wider, within the bound.
A program may use at most 128 MiB of HBM per device.

```python
import math
import jax
import jax.numpy as jnp
import numpy as np
from jax import lax

FEATURE_SPAN = 4096
H = 64
HEAD = 64
FF = 16384
VOCAB = 65536
RW = 128
RA = 128
RG = 480
BATCH = 256


def draw_lexicon_table(key, part):
    key_values, key_scales = jax.random.split(key, 2)
    position = jnp.arange(FEATURE_SPAN, dtype=jnp.float32) / FEATURE_SPAN
    column_scale = jnp.exp(jax.random.uniform(key_scales, (FEATURE_SPAN,), jnp.float32, 0.0, math.log(10.0)) + math.log(3.0) * position) / 3.0
    entries = jax.random.truncated_normal(key_values, -4.0, 4.0, (VOCAB, FEATURE_SPAN), jnp.float32)
    return (entries * column_scale).astype(jnp.bfloat16)


def plant(array, rng, smallest, largest):
    extent = array.shape
    spot = [jax.random.randint(jax.random.fold_in(rng, axis), (), 0, extent[axis]) for axis in range(len(extent))]
    array = array.at[tuple(spot)].set(smallest)
    longest = extent.index(max(extent))
    spot[longest] = (spot[longest] + 1) % extent[longest]
    return array.at[tuple(spot)].set(largest)


def strengthened(drawn, rng, source, target, shards_of, factor):
    owner, partner = [(jnp.arange(drawn.shape[dim]) // (drawn.shape[dim] // shards_of)).reshape([-1 if axis == dim else 1 for axis in range(drawn.ndim)]) for dim in (source, target)]
    chosen = jax.random.permutation(rng, shards_of)[partner]
    strong = (owner == chosen) | (owner == (partner + shards_of // 2) % shards_of)
    return jnp.where(strong, factor * drawn, drawn)


def block_scale(rng, extent, shards, smallest, high):
    factor_of = 1.0
    for dim, parts in shards:
        steps = jax.random.uniform(jax.random.fold_in(jax.random.fold_in(rng, 6), dim), (parts,), jnp.float32, smallest / len(shards), high / len(shards))
        factor_of = factor_of * jnp.repeat(jnp.exp(steps), extent[dim] // parts).reshape((-1,) + (1,) * (len(extent) - 1 - dim))
    return factor_of


def rank_bounds(count, lean):
    loads = [(1 << 20) // math.isqrt(grade ** lean) + 1 for grade in range(1, count + 1)]
    deviation = 1 + sum(loads) // (1 << 30)
    return np.cumsum(np.array([max(1, weight // deviation) for weight in loads]))


def ranked(rng, extent, number_of, lean):
    table = rank_bounds(number_of, lean)
    ticket = jax.random.randint(jax.random.fold_in(rng, 1), extent, 0, int(table[number_of - 1]))
    rank = jnp.searchsorted(jnp.asarray(table, jnp.int32), ticket, side="right")
    return jax.random.permutation(jax.random.fold_in(rng, 2), number_of)[rank].astype(jnp.int32)


def noise(own_key, shape, spread, limit, cuts=(), held_as=jnp.bfloat16):
    result = jax.random.normal(own_key, shape, jnp.float32) * spread
    if len(cuts) > 0:
        result = block_scale(own_key, shape, cuts, -0.22, 0.18) * result
    return jnp.clip(result, min=-limit, max=limit).astype(held_as)


def gaussian_with(own_key, extent, deviation, most, pieces, heavy, kind=jnp.bfloat16):
    array = deviation * jax.random.normal(own_key, extent, jnp.float32)
    if pieces:
        array = array * block_scale(own_key, extent, pieces, -0.22, 0.18)
    return jnp.clip(strengthened(array, jax.random.fold_in(own_key, 3), *heavy), -most, most).astype(kind)


def setup_inputs(seed: int = 0) -> dict:
    key_of = jax.random.split(jax.random.key(seed), 33)
    return {
        "latest_symbol_ids": plant(ranked(key_of[0], (BATCH,), VOCAB, 2), jax.random.fold_in(key_of[0], 3), 0, VOCAB - 1).astype(jnp.int32),
        "lexicon_table": draw_lexicon_table(jax.random.fold_in(key_of[32], 71), 0),
        "lexicon_layernorm_stretch": jnp.clip(jnp.exp(math.log(3.0) - 2.306499 * jax.random.uniform(key_of[2], (FEATURE_SPAN,), jnp.float32) ** block_scale(key_of[2], (FEATURE_SPAN,), ((0, 32),), -0.2, 0.2)), 0.29882812, 3.0).astype(jnp.bfloat16),
        "lexicon_layernorm_shift": noise(key_of[3], (FEATURE_SPAN,), 0.3, 4.0, ((0, 32),)),
        "recurrent_layernorm_stretch": jnp.clip(1.0 + 0.15 * jax.random.normal(key_of[4], (FEATURE_SPAN,), jnp.float32), 0.25, 1.75).astype(jnp.bfloat16),
        "recurrent_layernorm_shift": noise(key_of[5], (FEATURE_SPAN,), 0.2, 3.0, ((0, 32),)),
        "prior_recurrent_signal": noise(key_of[6], (BATCH, FEATURE_SPAN), 1.0, 6.0, ((0, 4), (1, 32))),
        "recurrent_lerp_coefs": jnp.clip(1.0 * jax.random.uniform(key_of[7], (6, FEATURE_SPAN), jnp.float32) ** block_scale(key_of[7], (6, FEATURE_SPAN), ((1, 32),), -0.2, 0.2), 0.0, 1.0).astype(jnp.bfloat16),
        "forgetting_lowrank_first": noise(key_of[8], (FEATURE_SPAN, RW), FEATURE_SPAN ** -0.5, 0.09375, ((0, 32),)),
        "forgetting_lowrank_second": noise(key_of[9], (RW, FEATURE_SPAN), RW ** -0.5, 0.5, ((1, 32),)),
        "forgetting_baseline": jnp.clip(-5.0 + 6.0 * jax.random.uniform(key_of[10], (FEATURE_SPAN,), jnp.float32) ** block_scale(key_of[10], (FEATURE_SPAN,), ((0, 32),), -0.2, 0.2), -5.0, 1.0).astype(jnp.bfloat16),
        "learning_speed_lowrank_first": noise(key_of[11], (FEATURE_SPAN, RA), FEATURE_SPAN ** -0.5, 0.09375, ((0, 32),)),
        "learning_speed_lowrank_second": noise(key_of[12], (RA, FEATURE_SPAN), RA ** -0.5, 0.5, ((1, 32),)),
        "learning_speed_baseline": jnp.clip(jax.random.uniform(key_of[13], (FEATURE_SPAN,), jnp.float32, -2.0, 2.0) * block_scale(key_of[13], (FEATURE_SPAN,), ((0, 32),), -0.4, 0.0), -2.0, 2.0).astype(jnp.bfloat16),
        "valve_lowrank_first": noise(key_of[14], (FEATURE_SPAN, RG), FEATURE_SPAN ** -0.5, 0.09375, ((0, 32),)),
        "valve_lowrank_second": noise(key_of[15], (RG, FEATURE_SPAN), RG ** -0.5, 0.25, ((1, 32),)),
        "erasure_lookup_coefs": jnp.clip(0.5 + 1.0 * jax.random.uniform(key_of[16], (FEATURE_SPAN,), jnp.float32) ** block_scale(key_of[16], (FEATURE_SPAN,), ((0, 32),), -0.2, 0.2), 0.5, 1.5).astype(jnp.bfloat16),
        "lookup_speed_coefs": jnp.clip(0.5 + 1.0 * jax.random.uniform(key_of[17], (FEATURE_SPAN,), jnp.float32) ** block_scale(key_of[17], (FEATURE_SPAN,), ((0, 32),), -0.2, 0.2), 0.5, 1.5).astype(jnp.bfloat16),
        "present_reward_coefs": noise(key_of[18], (FEATURE_SPAN,), 0.3, 4.0, ((0, 32),)),
        "acceptance_projection": noise(key_of[19], (FEATURE_SPAN, FEATURE_SPAN), FEATURE_SPAN ** -0.5, 0.09375, ((1, 32),)),
        "lookup_projection": noise(key_of[20], (FEATURE_SPAN, FEATURE_SPAN), FEATURE_SPAN ** -0.5, 0.09375, ((1, 32),)),
        "payload_projection": noise(key_of[21], (FEATURE_SPAN, FEATURE_SPAN), FEATURE_SPAN ** -0.5, 0.09375, ((1, 32),)),
        "memory_tensor": noise(key_of[22], (BATCH, H, HEAD, HEAD), 0.5, 6.0, ((0, 4), (1, 32)), jnp.float32),
        "cluster_layernorm_stretch": jnp.clip(1.0 + 0.15 * jax.random.normal(key_of[23], (FEATURE_SPAN,), jnp.float32), 0.25, 1.75).astype(jnp.bfloat16),
        "cluster_layernorm_shift": noise(key_of[24], (FEATURE_SPAN,), 0.2, 3.0, ((0, 32),)),
        "recurrent_result_proj": gaussian_with(key_of[25], (FEATURE_SPAN, FEATURE_SPAN), FEATURE_SPAN ** -0.5, 0.1875, ((0, 32),), (0, 1, 32, 2.75)),
        "feedforward_layernorm_stretch": jnp.clip(1.0 + 0.15 * jax.random.normal(key_of[26], (FEATURE_SPAN,), jnp.float32), 0.25, 1.75).astype(jnp.bfloat16),
        "feedforward_layernorm_shift": noise(key_of[27], (FEATURE_SPAN,), 0.2, 3.0, ((0, 32),)),
        "prior_feedforward_signal": noise(key_of[28], (BATCH, FEATURE_SPAN), 1.0, 6.0, ((0, 4), (1, 32))),
        "feedforward_lerp_coefs": jnp.clip(1.0 * jax.random.uniform(key_of[29], (FEATURE_SPAN,), jnp.float32) ** block_scale(key_of[29], (FEATURE_SPAN,), ((0, 32),), -0.2, 0.2), 0.0, 1.0).astype(jnp.bfloat16),
        "feedforward_lookup_proj": noise(key_of[30], (FEATURE_SPAN, FF), FEATURE_SPAN ** -0.5, 0.09375, ((1, 32),)),
        "feedforward_payload_proj": gaussian_with(key_of[31], (FF, FEATURE_SPAN), FF ** -0.5, 0.09375, ((0, 32),), (0, 1, 32, 2.75)),
    }


def matmul(left, right):
    return jnp.dot(left, right, preferred_element_type=jnp.float32)

def layer_norm(inputs, norm_gain, norm_bias):
    row_mean = lax.optimization_barrier(jnp.mean(inputs, axis=-1, keepdims=True))
    row_var = lax.optimization_barrier(jnp.mean(jnp.square(inputs - row_mean), axis=-1, keepdims=True))
    return (inputs - row_mean) * lax.rsqrt(row_var + 1e-05) * norm_gain.astype(jnp.float32) + norm_bias.astype(jnp.float32)

def recurrent_kernel(acceptance_vectors, raw_lookups, payload_vectors, forgetting_multiplier, learning_speed, result_valve, memory_tensor, erasure_lookup_coefs, lookup_speed_coefs, present_reward_coefs, cluster_layernorm_stretch, cluster_layernorm_shift):
    sequence_number = memory_tensor.shape[0]
    attention_parts = memory_tensor.shape[1]
    attention_span = memory_tensor.shape[2]
    regrouped_vectors = (sequence_number, attention_parts, attention_span)
    recept_heads = acceptance_vectors.reshape(regrouped_vectors)
    payload_each_part = payload_vectors.reshape(regrouped_vectors)
    decay_heads = forgetting_multiplier.reshape(regrouped_vectors)
    alpha_heads = learning_speed.reshape(regrouped_vectors)
    removal_key = (raw_lookups * erasure_lookup_coefs.astype(jnp.float32)).reshape(regrouped_vectors)
    removal_key = removal_key * lax.rsqrt(lax.optimization_barrier(jnp.sum(removal_key * removal_key, axis=-1, keepdims=True)) + 1e-06)
    stored_lookup_vectors = raw_lookups * (1.0 + (learning_speed - 1.0) * lookup_speed_coefs.astype(jnp.float32))
    added_heads = stored_lookup_vectors.reshape(regrouped_vectors)
    removed = lax.optimization_barrier(jnp.sum(memory_tensor * removal_key[:, :, None, :], axis=-1))
    new_state = memory_tensor * decay_heads[:, :, None, :] - removed[:, :, :, None] * (removal_key * alpha_heads)[:, :, None, :] + payload_each_part[:, :, :, None] * added_heads[:, :, None, :]
    readout = lax.optimization_barrier(jnp.sum(new_state * recept_heads[:, :, None, :], axis=-1))
    head_mean = lax.optimization_barrier(jnp.mean(readout, axis=-1, keepdims=True))
    head_var = lax.optimization_barrier(jnp.mean(jnp.square(readout - head_mean), axis=-1, keepdims=True))
    standardized_signal = ((readout - head_mean) * lax.rsqrt(head_var + 0.00064)).reshape(sequence_number, attention_parts * attention_span)
    standardized_signal = standardized_signal * cluster_layernorm_stretch.astype(jnp.float32) + cluster_layernorm_shift.astype(jnp.float32)
    present_reward = lax.optimization_barrier(jnp.sum((acceptance_vectors * stored_lookup_vectors * present_reward_coefs.astype(jnp.float32)).reshape(regrouped_vectors), axis=-1, keepdims=True)) * payload_each_part
    valved_result = (standardized_signal + present_reward.reshape(sequence_number, attention_parts * attention_span)) * result_valve
    return (valved_result.astype(jnp.bfloat16), new_state)

def reference(latest_symbol_ids, lexicon_table, lexicon_layernorm_stretch, lexicon_layernorm_shift, recurrent_layernorm_stretch, recurrent_layernorm_shift, prior_recurrent_signal, recurrent_lerp_coefs, forgetting_lowrank_first, forgetting_lowrank_second, forgetting_baseline, learning_speed_lowrank_first, learning_speed_lowrank_second, learning_speed_baseline, valve_lowrank_first, valve_lowrank_second, erasure_lookup_coefs, lookup_speed_coefs, present_reward_coefs, acceptance_projection, lookup_projection, payload_projection, memory_tensor, cluster_layernorm_stretch, cluster_layernorm_shift, recurrent_result_proj, feedforward_layernorm_stretch, feedforward_layernorm_shift, prior_feedforward_signal, feedforward_lerp_coefs, feedforward_lookup_proj, feedforward_payload_proj):
    emb_rows = jnp.take(lexicon_table, latest_symbol_ids, axis=0).astype(jnp.float32)
    residual = layer_norm(emb_rows, lexicon_layernorm_stretch, lexicon_layernorm_shift)
    att_in = layer_norm(residual, recurrent_layernorm_stretch, recurrent_layernorm_shift).astype(jnp.bfloat16)
    att_base = att_in.astype(jnp.float32)
    shift_delta = prior_recurrent_signal.astype(jnp.float32) - att_base
    mixed = [(att_base + shift_delta * recurrent_lerp_coefs[column].astype(jnp.float32)).astype(jnp.bfloat16) for column in range(6)]
    acceptance_vectors = matmul(mixed[0], acceptance_projection)
    raw_lookups = matmul(mixed[2], lookup_projection)
    payload_vectors = matmul(mixed[3], payload_projection)
    decay_low = jnp.tanh(matmul(mixed[1], forgetting_lowrank_first)).astype(jnp.bfloat16)
    alpha_low = matmul(mixed[4], learning_speed_lowrank_first).astype(jnp.bfloat16)
    gate_low = jax.nn.sigmoid(matmul(mixed[5], valve_lowrank_first)).astype(jnp.bfloat16)
    decay_log = -jax.nn.softplus(-(forgetting_baseline.astype(jnp.float32) + matmul(decay_low, forgetting_lowrank_second))) - 0.5
    forgetting_multiplier = jnp.exp(-jnp.exp(decay_log))
    learning_speed = jax.nn.sigmoid(learning_speed_baseline.astype(jnp.float32) + matmul(alpha_low, learning_speed_lowrank_second))
    result_valve = matmul(gate_low, valve_lowrank_second)
    recurrent_result, refreshed_memory = recurrent_kernel(acceptance_vectors, raw_lookups, payload_vectors, forgetting_multiplier, learning_speed, result_valve, memory_tensor, erasure_lookup_coefs, lookup_speed_coefs, present_reward_coefs, cluster_layernorm_stretch, cluster_layernorm_shift)
    midway = residual + matmul(recurrent_result, recurrent_result_proj)
    ffn_in = layer_norm(midway, feedforward_layernorm_stretch, feedforward_layernorm_shift).astype(jnp.bfloat16)
    ffn_base = ffn_in.astype(jnp.float32)
    ffn_input = (ffn_base + (prior_feedforward_signal.astype(jnp.float32) - ffn_base) * feedforward_lerp_coefs.astype(jnp.float32)).astype(jnp.bfloat16)
    hidden = jnp.square(jax.nn.relu(matmul(ffn_input, feedforward_lookup_proj))).astype(jnp.bfloat16)
    hidden_out = midway + matmul(hidden, feedforward_payload_proj)
    return (hidden_out, refreshed_memory, att_in, ffn_in, payload_vectors.astype(jnp.bfloat16))
```

```python
import jax
import jax.numpy as jnp
from jax import lax
from jax.experimental import pallas as pl
from jax.experimental.pallas import tpu as pltpu
from jax.sharding import PartitionSpec as P

MESH = pl.DeviceIdType.MESH
F32 = jnp.float32
BF16 = jnp.bfloat16
N = 4096
NQ = 16
NM = 32
ND = 4
LOW = 23
V_RK, V_DR, V_D, V_RKA, V_W, V_V, V_REM = range(7)
E_HALF = 0.6065306597126334


def whole_step(
    ids, table, prior_rec, lerp, wd1, wd2, wa1, wa2, wg1, wg2, wr, wk, wv, state, wo, prior_ffn, wup, wdn,
    g1, b1, g2, b2, g3, b3, lerp_ffn, fbase, abase, erase, lcoef, reward, clg, clb,
    out_h, out_s, out_att, out_ffn, out_v,
    idv, ids_s, tab, prm, lerp_v, wd1_v, wd2_v, wa1_v, wa2_v, wg1_v, wg2_v, wr_v, wk_v, wv_v, s_v,
    wop, wup_v, wdp, rows_s, rows_r, abuf, ebuf, fbuf, mbuf, wts, wt, mx, res, lt, vec, rowb, ap, zf, zs, zr, zs2, zr2, hp,
    ov_h, ov_att, ov_ffn, ov_v,
    ld, zsem, asem, esem, fsem, msem, wsem, wrecv, ltsend, ltrecv, psem, z1sem, z2sem, hsem, osem,
):
    d = lax.axis_index("dp")
    me = lax.axis_index("mp")
    q = me // 2
    c = me % 2
    mate = me + 1 - 2 * c

    def remote(src, dst, ssem, rsem, dev):
        return pltpu.make_async_remote_copy(
            src_ref=src, dst_ref=dst, send_sem=ssem, recv_sem=rsem, device_id=dev, device_id_type=MESH
        )

    def lanes(i):
        return pl.ds(pl.multiple_of(i * 128, 128), 128)

    loads = []

    def load(src, dst):
        k = pltpu.make_async_copy(src, dst, ld.at[len(loads)])
        k.start()
        loads.append(k)
        return k

    l_ids = load(ids, idv.at[d])
    l_prm = [
        load(p, prm.at[i])
        for i, p in enumerate((g1, b1, g2, b2, g3, b3, lerp_ffn, fbase, abase, erase, lcoef, reward, clg, clb))
    ]
    l_prm.append(load(lerp, lerp_v))
    l_prior = load(prior_rec, abuf.at[c, q, pl.ds(16, 64), :])
    l_low = [load(wd1, wd1_v), load(wa1, wa1_v), load(wg1, wg1_v)]
    l_tab = load(table, tab)
    l_rkv = [load(wk, wk_v), load(wv, wv_v), load(wr, wr_v)]
    l_s = load(state, s_v)
    l_low2 = [load(wd2, wd2_v), load(wa2, wa2_v), load(wg2, wg2_v)]
    l_priorf = load(prior_ffn, fbuf.at[c, q])

    barrier = pltpu.get_barrier_semaphore()

    @pl.loop(1, ND)
    def _(i):
        pl.semaphore_signal(barrier, inc=1, device_id=((d + i) % ND, me), device_id_type=MESH)

    @pl.loop(1, NM)
    def _(i):
        pl.semaphore_signal(barrier, inc=1, device_id=(d, (me + i) % NM), device_id_type=MESH)

    for k in l_prm:
        k.wait()
    par = lambda i: prm[i].astype(F32)
    lerp_own = lerp_v[...].astype(F32)
    packed = jnp.concatenate(
        [par(0), par(1), par(2), par(3), lerp_own, par(4), par(5), par(6), jnp.zeros((3, 128), F32)], axis=0
    )
    abuf[c, q, 0:16, :] = packed.astype(BF16)
    for k in l_low:
        k.wait()
    wts[0:128, :] = jnp.transpose(wd1_v[...].astype(F32)).astype(BF16)
    wts[128:256, :] = jnp.transpose(wa1_v[...].astype(F32)).astype(BF16)
    for t in range(3):
        wts[256 + 128 * t : 384 + 128 * t, :] = jnp.transpose(
            wg1_v[:, 128 * t : 128 * t + 128].astype(F32)
        ).astype(BF16)
    wts[640:736, :] = jnp.transpose(wg1_v[:, 384:480].astype(F32)).astype(BF16)
    l_ids.wait()
    l_prior.wait()

    pl.semaphore_wait(barrier, ND - 1 + NM - 1)

    @pl.loop(1, ND)
    def _(i):
        remote(idv.at[d], idv.at[d], zsem.at[0], zsem.at[1], ((d + i) % ND, me)).start()

    def gather_start(buf, sem):
        @pl.loop(1, NQ)
        def _(i):
            remote(buf.at[c, q], buf.at[c, q], sem.at[0], sem.at[1], (d, 2 * ((q + i) % NQ) + c)).start()

    def gather_finish(buf, sem):
        part = buf.at[0, pl.ds(0, NQ - 1)]
        remote(part, part, sem.at[0], sem.at[1], (d, mate)).wait_recv()
        k = remote(buf.at[c], buf.at[c], sem.at[2], sem.at[3], (d, mate))
        k.start()
        return k

    def gather_sent(buf, sem):
        part = buf.at[0, pl.ds(0, NQ - 1)]
        remote(part, part, sem.at[0], sem.at[1], (d, mate)).wait_send()

    gather_start(abuf, asem)

    @pl.loop(0, LOW)
    def _(j):
        @pl.when(j != me)
        def _():
            remote(
                wts.at[pl.ds(pl.multiple_of(j * 32, 32), 32), :], wt.at[:, lanes(me)], wsem.at[j], wrecv, (d, j)
            ).start()

    @pl.when(me < LOW)
    def _():
        wt[:, lanes(me)] = wts[pl.ds(pl.multiple_of(me * 32, 32), 32), :]

    own_w = []
    for t in range(NQ):
        own_w.append(
            (
                pltpu.make_async_copy(
                    wo.at[:, lanes(2 * t + c)],
                    wop.at[pl.ds(pl.multiple_of(c * 128, 128), 128), pl.ds(t * 128, 128)],
                    psem.at[0],
                ),
                remote(
                    wo.at[:, lanes(2 * t + 1 - c)],
                    wop.at[pl.ds(pl.multiple_of(c * 128, 128), 128), pl.ds(t * 128, 128)],
                    psem.at[1],
                    psem.at[2],
                    (d, mate),
                ),
                pltpu.make_async_copy(
                    wdn.at[:, lanes(2 * t + c)],
                    wdp.at[pl.ds(pl.multiple_of(c * 512, 512), 512), pl.ds(t * 128, 128)],
                    psem.at[3],
                ),
                remote(
                    wdn.at[:, lanes(2 * t + 1 - c)],
                    wdp.at[pl.ds(pl.multiple_of(c * 512, 512), 512), pl.ds(t * 128, 128)],
                    psem.at[4],
                    psem.at[5],
                    (d, mate),
                ),
            )
        )
    for k in own_w:
        k[0].start()
        k[1].start()
    l_up = load(wup, wup_v)
    for k in own_w:
        k[2].start()
        k[3].start()

    part = idv.at[pl.ds(0, ND - 1)]
    remote(part, part, zsem.at[0], zsem.at[1], (d, mate)).wait_recv()
    k = pltpu.make_async_copy(idv, ids_s, ld.at[len(loads)])
    k.start()
    l_tab.wait()
    k.wait()
    base = d * tab.shape[0] * 8
    sub8 = lax.broadcasted_iota(jnp.int32, (8, 128), 0)

    for s in range(ND):
        @pl.loop(0, 8)
        def _(g, s=s):
            block = jnp.zeros((8, 128), F32)
            for u in range(8):
                at = ids_s[s, 0, g * 8 + u] - base
                inside = jnp.logical_and(at >= 0, at < tab.shape[0] * 8)
                at = jnp.where(inside, at, 0)
                eight = tab[at // 8].astype(F32)
                want = jnp.where(inside, at % 8, 8)
                row = jnp.sum(jnp.where(sub8 == want, eight, 0.0), axis=0, keepdims=True)
                block = jnp.where(sub8 == u, row, block)
            rowb[0, pl.ds(pl.multiple_of(g * 8, 8), 8), :] = block

        rows_s[s] = rowb[0].astype(BF16)

        @pl.when(d != s)
        def _(s=s):
            remote(rows_s.at[s], rows_r.at[d], zsem.at[2], zsem.at[3], (s, me)).start()

    for s in range(ND):
        @pl.when(d == s)
        def _(s=s):
            rows_r[s] = rows_s[s]

    a_fwd = gather_finish(abuf, asem)

    part = rows_r.at[pl.ds(0, ND - 1)]
    remote(part, part, zsem.at[2], zsem.at[3], (d, mate)).wait_recv()
    found = rows_r[0].astype(F32)
    for s in range(1, ND):
        found = found + rows_r[s].astype(F32)
    ebuf[c, q] = found.astype(BF16)
    gather_start(ebuf, esem)
    l_priorf.wait()
    gather_start(fbuf, fsem)
    e_fwd = gather_finish(ebuf, esem)
    a_fwd.wait_recv()
    e_fwd.wait_recv()

    def params(cc, t):
        return abuf[cc, t, 0:16, :].astype(F32)

    zero = jnp.zeros((64, 128), F32)

    def over_blocks(body, init):
        def step(t, acc):
            for cc in (0, 1):
                acc = body(cc, t, acc)
            return acc

        return lax.fori_loop(0, NQ, step, init)

    def rowsum(x):
        return jnp.sum(x, axis=-1, keepdims=True)

    mean1 = rowsum(over_blocks(lambda cc, t, acc: acc + ebuf[cc, t].astype(F32), zero)) / N
    inv1 = lax.rsqrt(
        rowsum(over_blocks(lambda cc, t, acc: acc + jnp.square(ebuf[cc, t].astype(F32) - mean1), zero)) / N + 1e-05
    )

    def first_norm(cc, t, acc):
        p = params(cc, t)
        r = (ebuf[cc, t].astype(F32) - mean1) * inv1 * p[0:1] + p[1:2]
        res[cc, t] = r
        return acc + r

    mean2 = rowsum(over_blocks(first_norm, zero)) / N
    inv2 = lax.rsqrt(rowsum(over_blocks(lambda cc, t, acc: acc + jnp.square(res[cc, t] - mean2), zero)) / N + 1e-05)

    def mixing(cc, t, acc):
        p = params(cc, t)
        att = ((res[cc, t] - mean2) * inv2 * p[2:3] + p[3:4]).astype(BF16).astype(F32)
        delta = abuf[cc, t, 16:80, :].astype(F32) - att
        low = jnp.where(me < 4, p[5:6], jnp.where(me < 8, p[8:9], p[9:10]))
        at = lanes(2 * t + cc)
        mx[0, :, at] = (att + delta * low).astype(BF16)
        mx[1, :, at] = (att + delta * p[6:7]).astype(BF16)
        mx[2, :, at] = (att + delta * p[7:8]).astype(BF16)
        mx[3, :, at] = (att + delta * p[4:5]).astype(BF16)
        return acc

    over_blocks(mixing, 0)
    own_res = res[c, q]
    ov_att[...] = ((own_res - mean2) * inv2 * par(2) + par(3)).astype(BF16)
    outs = [pltpu.make_async_copy(ov_att, out_att, osem.at[0])]
    outs[0].start()

    @pl.when(me < LOW)
    def _():
        got = wt.at[:, pl.ds(0, (NM - 1) * 128)]
        remote(got, got, wsem.at[0], wrecv, (d, mate)).wait_recv()
        low = lax.dot_general(wt[...], mx[0], (((1,), (1,)), ((), ())), preferred_element_type=F32)
        low = jnp.where(me < 4, jnp.tanh(low), jnp.where(me < 8, low, jax.nn.sigmoid(low)))
        lt[me] = low.astype(BF16)

        @pl.loop(1, NM)
        def _(i):
            remote(lt.at[me], lt.at[me], ltsend, ltrecv.at[me], (d, (me + i) % NM)).start()

    def head_rows(i, x):
        vec[i, 0] = x
        vec[i, 1] = pltpu.roll(x, 64, axis=1)

    left = lax.broadcasted_iota(jnp.int32, (64, 128), 1) < 64
    eye = lax.broadcasted_iota(jnp.int32, (64, 64), 0) == lax.broadcasted_iota(jnp.int32, (64, 64), 1)

    def headsum(x):
        return jnp.where(left, rowsum(jnp.where(left, x, 0.0)), rowsum(jnp.where(left, 0.0, x)))

    def projected(i, w, k):
        k.wait()
        return jnp.dot(mx[i], w[...], preferred_element_type=F32)

    def state_times(i):
        @pl.loop(0, 64)
        def _(b):
            for h in (0, 1):
                col = rowsum(s_v[b, h] * vec[i, h, pl.ds(b, 1), 0:64])
                rowb[h, pl.ds(b, 1), 0:64] = jnp.sum(jnp.where(eye, col, 0.0), axis=0, keepdims=True)

        return jnp.where(left, rowb[0], pltpu.roll(rowb[1], 64, axis=1))

    keys = projected(1, wk_v, l_rkv[0])
    removal = keys * par(9)
    removal = removal * lax.rsqrt(headsum(removal * removal) + 1e-06)
    values = projected(2, wv_v, l_rkv[1])
    recept = projected(3, wr_v, l_rkv[2])
    ov_v[...] = values.astype(BF16)
    outs.append(pltpu.make_async_copy(ov_v, out_v, osem.at[1]))
    outs[1].start()
    head_rows(V_RK, removal)
    head_rows(V_V, values)
    rowb[0] = zero
    rowb[1] = zero
    l_s.wait()
    removed = state_times(V_RK)
    head_rows(V_REM, removed)

    for k in l_low2:
        k.wait()

    @pl.loop(0, LOW)
    def _(j):
        @pl.when(j != me)
        def _():
            remote(lt.at[j], lt.at[j], ltsend, ltrecv.at[j], (d, mate)).wait_recv()

    def second(lo, hi, w):
        low = lt[lo:hi].astype(F32).reshape((hi - lo) * 32, 64)
        return jnp.dot(jnp.transpose(low).astype(BF16), w[...], preferred_element_type=F32)

    decay = jnp.exp(-E_HALF * jax.nn.sigmoid(par(7) + second(0, 4, wd2_v)))
    alpha = jax.nn.sigmoid(par(8) + second(4, 8, wa2_v))
    gate = second(8, LOW, wg2_v)
    written = keys * (1.0 + (alpha - 1.0) * par(10))
    rka = removal * alpha
    head_rows(V_D, decay)
    head_rows(V_RKA, rka)
    head_rows(V_W, written)
    head_rows(V_DR, decay * recept)
    readout = (
        state_times(V_DR) - removed * headsum(rka * recept) + values * headsum(written * recept)
    )
    centered = readout - headsum(readout) / 64
    normed = centered * lax.rsqrt(headsum(centered * centered) / 64 + 0.00064) * par(12) + par(13)
    bonus = headsum(recept * written * par(11)) * values
    ap[c] = ((normed + bonus) * gate).astype(BF16)
    k = remote(ap.at[c], ap.at[c], hsem.at[0], hsem.at[1], (d, mate))
    k.start()

    wo_own = wop.at[pl.ds(0, 128), :]
    pltpu.make_async_copy(wo_own, wo_own, psem.at[0]).wait()
    remote(wo_own, wo_own, psem.at[1], psem.at[2], (d, mate)).wait_recv()
    k.wait()

    def scatter(pair, w, send, recv, sem):
        @pl.loop(0, NQ // 2)
        def _(i):
            t = (i + q // 2) % (NQ // 2)
            y = jnp.dot(
                pair, w[:, pl.ds(pl.multiple_of(t * 256, 256), 256)], preferred_element_type=F32
            )
            for u in (0, 1):
                to = 2 * t + u
                block = y[:, 128 * u : 128 * u + 128]
                send[to] = block.astype(BF16)

                @pl.when(to != q)
                def _(to=to):
                    remote(send.at[to], recv.at[q], sem.at[0], sem.at[1], (d, 2 * to + c)).start()

                @pl.when(to == q)
                def _(block=block):
                    zf[...] = block
                    recv[q] = jnp.zeros((64, 128), BF16)

    def arrived(recv, sem):
        part = recv.at[pl.ds(0, NQ - 1)]
        remote(part, part, sem.at[0], sem.at[1], (d, mate)).wait_recv()
        total = zf[...]
        for t in range(NQ):
            total = total + recv[t].astype(F32)
        return total

    scatter(jnp.concatenate([ap[0], ap[1]], axis=1), wop, zs, zr, z1sem)

    @pl.loop(0, 64)
    def _(b):
        for h in (0, 1):
            row = lambda i: vec[i, h, pl.ds(b, 1), 0:64]
            gone = rowsum(jnp.where(eye, row(V_REM), 0.0))
            val = rowsum(jnp.where(eye, row(V_V), 0.0))
            s_v[b, h] = s_v[b, h] * row(V_D) - gone * row(V_RKA) + val * row(V_W)

    outs.append(pltpu.make_async_copy(s_v, out_s, osem.at[2]))
    outs[2].start()

    f_fwd = gather_finish(fbuf, fsem)
    midway = own_res + arrived(zr, z1sem)
    mbuf[c, q] = midway.astype(BF16)
    gather_start(mbuf, msem)
    f_fwd.wait_recv()
    m_fwd = gather_finish(mbuf, msem)
    m_fwd.wait_recv()

    mean3 = rowsum(over_blocks(lambda cc, t, acc: acc + mbuf[cc, t].astype(F32), zero)) / N
    inv3 = lax.rsqrt(
        rowsum(over_blocks(lambda cc, t, acc: acc + jnp.square(mbuf[cc, t].astype(F32) - mean3), zero)) / N + 1e-05
    )

    def ffn_mixing(cc, t, acc):
        p = params(cc, t)
        base = ((mbuf[cc, t].astype(F32) - mean3) * inv3 * p[10:11] + p[11:12]).astype(BF16).astype(F32)
        mx[0, :, lanes(2 * t + cc)] = (base + (fbuf[cc, t].astype(F32) - base) * p[12:13]).astype(BF16)
        return acc

    over_blocks(ffn_mixing, 0)
    l_up.wait()
    up = jnp.dot(mx[0], wup_v[...], preferred_element_type=F32)
    hp[c] = jnp.square(jnp.maximum(up, 0.0)).astype(BF16)
    k = remote(hp.at[c], hp.at[c], hsem.at[2], hsem.at[3], (d, mate))
    k.start()
    ov_ffn[...] = ((midway - mean3) * inv3 * par(4) + par(5)).astype(BF16)
    outs.append(pltpu.make_async_copy(ov_ffn, out_ffn, osem.at[3]))
    outs[3].start()
    wdn_own = wdp.at[pl.ds(0, 512), :]
    pltpu.make_async_copy(wdn_own, wdn_own, psem.at[3]).wait()
    remote(wdn_own, wdn_own, psem.at[4], psem.at[5], (d, mate)).wait_recv()
    k.wait()
    scatter(jnp.concatenate([hp[0], hp[1]], axis=1), wdp, zs2, zr2, z2sem)
    ov_h[...] = midway + arrived(zr2, z2sem)
    outs.append(pltpu.make_async_copy(ov_h, out_h, osem.at[4]))
    outs[4].start()

    part = idv.at[pl.ds(0, ND - 1)]
    remote(part, part, zsem.at[0], zsem.at[1], (d, mate)).wait_send()
    part = rows_s.at[pl.ds(0, ND - 1)]
    remote(part, part, zsem.at[2], zsem.at[3], (d, mate)).wait_send()
    for buf, sem, k in ((abuf, asem, a_fwd), (ebuf, esem, e_fwd), (fbuf, fsem, f_fwd), (mbuf, msem, m_fwd)):
        gather_sent(buf, sem)
        k.wait_send()

    @pl.loop(0, LOW)
    def _(j):
        @pl.when(j != me)
        def _():
            piece = wts.at[pl.ds(0, 32), :]
            remote(piece, piece, wsem.at[j], wrecv, (d, mate)).wait_send()

    @pl.when(me < LOW)
    def _():
        part = lt.at[pl.ds(0, NM - 1)]
        remote(part, part, ltsend, ltrecv.at[0], (d, mate)).wait_send()

    remote(wo_own, wo_own, psem.at[1], psem.at[2], (d, mate)).wait_send()
    remote(wdn_own, wdn_own, psem.at[4], psem.at[5], (d, mate)).wait_send()
    for buf, sem in ((zs, z1sem), (zs2, z2sem)):
        part = buf.at[pl.ds(0, NQ - 1)]
        remote(part, part, sem.at[0], sem.at[1], (d, mate)).wait_send()
    for k in outs:
        k.wait()


def per_device(
    ids, table, g1, b1, g2, b2, prior_rec, lerp, wd1, wd2, fbase, wa1, wa2, abase, wg1, wg2, erase, lcoef, reward,
    wr, wk, wv, state, clg, clb, wo, g3, b3, prior_ffn, lerp_ffn, wup, wdn,
):
    line = lambda x: x.reshape(1, 128)
    vocab = table.shape[0]
    operands = (
        ids.reshape(1, 64), table.reshape(vocab // 8, 8, 128), prior_rec, lerp, wd1, wd2, wa1, wa2, wg1, wg2,
        wr, wk, wv, state, wo, prior_ffn, wup, wdn,
        *map(line, (g1, b1, g2, b2, g3, b3, lerp_ffn, fbase, abase, erase, lcoef, reward, clg, clb)),
    )
    vmem = pltpu.VMEM
    dma = pltpu.SemaphoreType.DMA
    scratch = [
        vmem((ND, 1, 64), jnp.int32), pltpu.SMEM((ND, 1, 64), jnp.int32), vmem((vocab // 8, 8, 128), BF16),
        vmem((14, 1, 128), BF16), vmem((6, 128), BF16),
        vmem((128, 128), BF16), vmem((128, 128), BF16), vmem((128, 128), BF16), vmem((128, 128), BF16),
        vmem((128, 480), BF16), vmem((480, 128), BF16),
        vmem((N, 128), BF16), vmem((N, 128), BF16), vmem((N, 128), BF16), vmem((64, 2, 64, 64), F32),
        vmem((256, 2048), BF16), vmem((N, 512), BF16), vmem((1024, 2048), BF16),
        vmem((ND, 64, 128), BF16), vmem((ND, 64, 128), BF16),
        vmem((2, NQ, 80, 128), BF16), vmem((2, NQ, 64, 128), BF16), vmem((2, NQ, 64, 128), BF16), vmem((2, NQ, 64, 128), BF16),
        vmem((736, 128), BF16), vmem((32, N), BF16), vmem((4, 64, N), BF16), vmem((2, NQ, 64, 128), F32),
        vmem((NM, 32, 64), BF16), vmem((7, 2, 64, 128), F32), vmem((2, 64, 128), F32),
        vmem((2, 64, 128), BF16), vmem((64, 128), F32),
        vmem((NQ, 64, 128), BF16), vmem((NQ, 64, 128), BF16), vmem((NQ, 64, 128), BF16), vmem((NQ, 64, 128), BF16),
        vmem((2, 64, 512), BF16),
        vmem((64, 128), F32), vmem((64, 128), BF16), vmem((64, 128), BF16), vmem((64, 128), BF16),
        dma((32,)), dma((4,)), dma((4,)), dma((4,)), dma((4,)), dma((4,)), dma((LOW,)), dma, dma, dma((LOW,)),
        dma((6,)), dma((2,)), dma((2,)), dma((4,)), dma((5,)),
    ]
    anywhere = pl.BlockSpec(memory_space=pl.ANY)
    return pl.pallas_call(
        whole_step,
        name="whole_step",
        out_shape=(
            jax.ShapeDtypeStruct((64, 128), F32),
            jax.ShapeDtypeStruct(state.shape, F32),
            jax.ShapeDtypeStruct((64, 128), BF16),
            jax.ShapeDtypeStruct((64, 128), BF16),
            jax.ShapeDtypeStruct((64, 128), BF16),
        ),
        in_specs=[anywhere] * len(operands),
        out_specs=[anywhere] * 5,
        scratch_shapes=scratch,
        compiler_params=pltpu.CompilerParams(
            collective_id=0, has_side_effects=True, vmem_limit_bytes=60 << 20
        ),
    )(*operands)


def solution(mesh):
    col = P(None, "mp")
    row = P("mp", None)
    one = P("mp")
    both = P("dp", "mp")
    return jax.shard_map(
        per_device,
        mesh=mesh,
        in_specs=(
            P("dp"), both, one, one, one, one, both, col, row, col, one, row, col, one, row, col, one, one, one,
            col, col, col, P("dp", "mp", None, None), one, one, row, one, one, both, one, col, row,
        ),
        out_specs=(both, P("dp", "mp", None, None), both, both, both),
        check_vma=False,
    )
```

```python
import jax
import jax.numpy as jnp
from jax import lax
from jax.experimental import pallas as pl
from jax.experimental.pallas import tpu as pltpu
from jax.sharding import PartitionSpec as P

MESH = pl.DeviceIdType.MESH
F32 = jnp.float32
BF16 = jnp.bfloat16
N = 4096
NQ = 16
NM = 32
ND = 4
LOW = 23
V_RK, V_DR, V_D, V_RKA, V_W, V_V, V_REM = range(7)
VMEM_GRANT = 62_767_104
E_HALF = 0.6065306597126334


def whole_step(
    ids, table, prior_rec, lerp, wd1, wd2, wa1, wa2, wg1, wg2, wr, wk, wv, state, wo, prior_ffn, wup, wdn,
    g1, b1, g2, b2, g3, b3, lerp_ffn, fbase, abase, erase, lcoef, reward, clg, clb,
    ov_h, out_s, ov_att, ov_ffn, ov_v,
    idv, ids_s, tab, prm, lerp_v, wd1_v, wd2_v, wa1_v, wa2_v, wg2_v, wr_v, wk_v, wv_v, s_v,
    wop, wup_v, wdp, rows_s, rows_r, abuf, ebuf, fbuf, mbuf, wts, wt, mx, res, lt, vec, rowb, ap, zf, zs, zr, zs2, zr2, hp,
    ld, zsem, asem, esem, fsem, msem, wsem, wrecv, ltsend, ltrecv, psem, z1sem, z2sem, hsem,
):
    d = lax.axis_index("dp")
    me = lax.axis_index("mp")
    q = me // 2
    c = me % 2
    mate = me + 1 - 2 * c

    def remote(src, dst, ssem, rsem, dev):
        return pltpu.make_async_remote_copy(
            src_ref=src, dst_ref=dst, send_sem=ssem, recv_sem=rsem, device_id=dev, device_id_type=MESH
        )

    def lanes(i):
        return pl.ds(pl.multiple_of(i * 128, 128), 128)

    loads = []

    def load(src, dst):
        k = pltpu.make_async_copy(src, dst, ld.at[len(loads)])
        k.start()
        loads.append(k)
        return k

    l_ids = load(ids, idv.at[d])
    l_prm = [
        load(p, prm.at[i])
        for i, p in enumerate((g1, b1, g2, b2, g3, b3, lerp_ffn, fbase, abase, erase, lcoef, reward, clg, clb))
    ]
    l_prm.append(load(lerp, lerp_v))
    l_prior = load(prior_rec, abuf.at[c, q, pl.ds(16, 64), :])
    l_low = [load(wd1, wd1_v), load(wa1, wa1_v), load(wg1, wts.at[pl.ds(256, 480), :])]
    l_tab = load(table, tab)
    l_rkv = [load(wk, wk_v), load(wv, wv_v), load(wr, wr_v)]
    l_s = load(state, s_v)
    l_low2 = [load(wd2, wd2_v), load(wa2, wa2_v), load(wg2, wg2_v)]
    l_priorf = load(prior_ffn, fbuf.at[c, q])

    barrier = pltpu.get_barrier_semaphore()

    @pl.loop(1, ND)
    def _(i):
        pl.semaphore_signal(barrier, inc=1, device_id=((d + i) % ND, me), device_id_type=MESH)

    @pl.loop(1, NM)
    def _(i):
        pl.semaphore_signal(barrier, inc=1, device_id=(d, (me + i) % NM), device_id_type=MESH)

    for k in l_prm:
        k.wait()
    par = lambda i: prm[i].astype(F32)
    lerp_own = lerp_v[...].astype(F32)
    packed = jnp.concatenate(
        [par(0), par(1), par(2), par(3), lerp_own, par(4), par(5), par(6), jnp.zeros((3, 128), F32)], axis=0
    )
    abuf[c, q, 0:16, :] = packed.astype(BF16)
    for k in l_low:
        k.wait()
    wts[0:128, :] = jnp.transpose(wd1_v[...].astype(F32)).astype(BF16)
    wts[128:256, :] = jnp.transpose(wa1_v[...].astype(F32)).astype(BF16)
    l_ids.wait()
    l_prior.wait()

    pl.semaphore_wait(barrier, ND - 1 + NM - 1)

    @pl.loop(1, ND)
    def _(i):
        remote(idv.at[d], idv.at[d], zsem.at[0], zsem.at[1], ((d + i) % ND, me)).start()

    def gather_start(buf, sem):
        @pl.loop(1, NQ)
        def _(i):
            remote(buf.at[c, q], buf.at[c, q], sem.at[0], sem.at[1], (d, 2 * ((q + i) % NQ) + c)).start()

    def gather_finish(buf, sem):
        part = buf.at[0, pl.ds(0, NQ - 1)]
        remote(part, part, sem.at[0], sem.at[1], (d, mate)).wait_recv()
        k = remote(buf.at[c], buf.at[c], sem.at[2], sem.at[3], (d, mate))
        k.start()
        return k

    def gather_sent(buf, sem):
        part = buf.at[0, pl.ds(0, NQ - 1)]
        remote(part, part, sem.at[0], sem.at[1], (d, mate)).wait_send()

    gather_start(abuf, asem)

    @pl.loop(0, LOW)
    def _(j):
        @pl.when(j != me)
        def _():
            remote(
                wts.at[pl.ds(pl.multiple_of(j * 32, 32), 32), :], wt.at[:, lanes(me)], wsem.at[j], wrecv, (d, j)
            ).start()

    @pl.when(me < LOW)
    def _():
        wt[:, lanes(me)] = wts[pl.ds(pl.multiple_of(me * 32, 32), 32), :]

    own_w = []
    for t in range(NQ):
        own_w.append(
            (
                pltpu.make_async_copy(
                    wo.at[:, lanes(2 * t + c)],
                    wop.at[pl.ds(pl.multiple_of(c * 128, 128), 128), pl.ds(t * 128, 128)],
                    psem.at[0],
                ),
                remote(
                    wo.at[:, lanes(2 * t + 1 - c)],
                    wop.at[pl.ds(pl.multiple_of(c * 128, 128), 128), pl.ds(t * 128, 128)],
                    psem.at[1],
                    psem.at[2],
                    (d, mate),
                ),
                pltpu.make_async_copy(
                    wdn.at[:, lanes(2 * t + c)],
                    wdp.at[pl.ds(pl.multiple_of(c * 512, 512), 512), pl.ds(t * 128, 128)],
                    psem.at[3],
                ),
                remote(
                    wdn.at[:, lanes(2 * t + 1 - c)],
                    wdp.at[pl.ds(pl.multiple_of(c * 512, 512), 512), pl.ds(t * 128, 128)],
                    psem.at[4],
                    psem.at[5],
                    (d, mate),
                ),
            )
        )
    for k in own_w:
        k[0].start()
        k[1].start()
    l_up = load(wup, wup_v)
    for k in own_w:
        k[2].start()
        k[3].start()

    part = idv.at[pl.ds(0, ND - 1)]
    remote(part, part, zsem.at[0], zsem.at[1], (d, mate)).wait_recv()
    k = pltpu.make_async_copy(idv, ids_s, ld.at[len(loads)])
    k.start()
    l_tab.wait()
    k.wait()
    base = d * tab.shape[0] * 8
    sub8 = lax.broadcasted_iota(jnp.int32, (8, 128), 0)

    for i in range(ND):
        s = (d + 1 + i) % ND

        @pl.loop(0, 8, unroll=4)
        def _(g, s=s, i=i):
            block = jnp.zeros((8, 128), F32)
            for u in range(8):
                at = ids_s[s, 0, g * 8 + u] - base
                inside = jnp.logical_and(at >= 0, at < tab.shape[0] * 8)
                at = jnp.where(inside, at, 0)
                eight = tab[at // 8].astype(F32)
                want = jnp.where(inside, at % 8, 8)
                row = jnp.sum(jnp.where(sub8 == want, eight, 0.0), axis=0, keepdims=True)
                block = jnp.where(sub8 == u, row, block)
            rowb[i % 2, pl.ds(pl.multiple_of(g * 8, 8), 8), :] = block

        if i < ND - 1:
            rows_s[s] = rowb[i % 2].astype(BF16)
            remote(rows_s.at[s], rows_r.at[d], zsem.at[2], zsem.at[3], (s, me)).start()
        else:
            rows_r[d] = rowb[i % 2].astype(BF16)

    a_fwd = gather_finish(abuf, asem)

    part = rows_r.at[pl.ds(0, ND - 1)]
    remote(part, part, zsem.at[2], zsem.at[3], (d, mate)).wait_recv()
    found = rows_r[0].astype(F32)
    for s in range(1, ND):
        found = found + rows_r[s].astype(F32)
    ebuf[c, q] = found.astype(BF16)
    gather_start(ebuf, esem)
    l_priorf.wait()
    gather_start(fbuf, fsem)
    e_fwd = gather_finish(ebuf, esem)
    a_fwd.wait_recv()
    e_fwd.wait_recv()

    def params(cc, t):
        return abuf[cc, t, 0:16, :].astype(F32)

    zero = jnp.zeros((64, 128), F32)

    def over_blocks(body, init):
        def step(t, acc):
            for cc in (0, 1):
                acc = body(cc, t, acc)
            return acc

        return lax.fori_loop(0, NQ, step, init)

    def rowsum(x):
        return jnp.sum(x, axis=-1, keepdims=True)

    mean1 = rowsum(over_blocks(lambda cc, t, acc: acc + ebuf[cc, t].astype(F32), zero)) / N
    inv1 = lax.rsqrt(
        rowsum(over_blocks(lambda cc, t, acc: acc + jnp.square(ebuf[cc, t].astype(F32) - mean1), zero)) / N + 1e-05
    )

    def first_norm(cc, t, acc):
        p = params(cc, t)
        r = (ebuf[cc, t].astype(F32) - mean1) * inv1 * p[0:1] + p[1:2]
        res[cc, t] = r
        return acc + r

    mean2 = rowsum(over_blocks(first_norm, zero)) / N
    inv2 = lax.rsqrt(rowsum(over_blocks(lambda cc, t, acc: acc + jnp.square(res[cc, t] - mean2), zero)) / N + 1e-05)

    def mixing(cc, t, acc):
        p = params(cc, t)
        att = ((res[cc, t] - mean2) * inv2 * p[2:3] + p[3:4]).astype(BF16).astype(F32)
        delta = abuf[cc, t, 16:80, :].astype(F32) - att
        low = jnp.where(me < 4, p[5:6], jnp.where(me < 8, p[8:9], p[9:10]))
        at = lanes(2 * t + cc)
        mx[0, :, at] = (att + delta * low).astype(BF16)
        mx[1, :, at] = (att + delta * p[6:7]).astype(BF16)
        mx[2, :, at] = (att + delta * p[7:8]).astype(BF16)
        mx[3, :, at] = (att + delta * p[4:5]).astype(BF16)
        return acc

    over_blocks(mixing, 0)
    own_res = res[c, q]
    ov_att[...] = ((own_res - mean2) * inv2 * par(2) + par(3)).astype(BF16)

    @pl.when(me < LOW)
    def _():
        got = wt.at[:, pl.ds(0, (NM - 1) * 128)]
        remote(got, got, wsem.at[0], wrecv, (d, mate)).wait_recv()
        low = lax.dot_general(wt[...], mx[0], (((1,), (1,)), ((), ())), preferred_element_type=F32)
        low = jnp.where(me < 4, jnp.tanh(low), jnp.where(me < 8, low, jax.nn.sigmoid(low)))
        lt[me] = low.astype(BF16)

        @pl.loop(1, NM)
        def _(i):
            remote(lt.at[me], lt.at[me], ltsend, ltrecv.at[me], (d, (me + i) % NM)).start()

    def head_rows(i, x):
        vec[i, 0] = x
        vec[i, 1] = pltpu.roll(x, 64, axis=1)

    left = lax.broadcasted_iota(jnp.int32, (64, 128), 1) < 64
    eye = lax.broadcasted_iota(jnp.int32, (64, 64), 0) == lax.broadcasted_iota(jnp.int32, (64, 64), 1)

    def headsum(x):
        return jnp.where(left, rowsum(jnp.where(left, x, 0.0)), rowsum(jnp.where(left, 0.0, x)))

    def projected(i, w, k):
        k.wait()
        return jnp.dot(mx[i], w[...], preferred_element_type=F32)

    def state_times(i):
        @pl.loop(0, 64, unroll=8)
        def _(b):
            for h in (0, 1):
                col = rowsum(s_v[b, h] * vec[i, h, pl.ds(b, 1), 0:64])
                rowb[h, pl.ds(b, 1), 0:64] = jnp.sum(jnp.where(eye, col, 0.0), axis=0, keepdims=True)

        return jnp.where(left, rowb[0], pltpu.roll(rowb[1], 64, axis=1))

    keys = projected(1, wk_v, l_rkv[0])
    removal = keys * par(9)
    removal = removal * lax.rsqrt(headsum(removal * removal) + 1e-06)
    values = projected(2, wv_v, l_rkv[1])
    recept = projected(3, wr_v, l_rkv[2])
    ov_v[...] = values.astype(BF16)
    head_rows(V_RK, removal)
    head_rows(V_V, values)
    rowb[0] = zero
    rowb[1] = zero
    l_s.wait()
    removed = state_times(V_RK)
    head_rows(V_REM, removed)

    for k in l_low2:
        k.wait()

    @pl.loop(0, LOW)
    def _(j):
        @pl.when(j != me)
        def _():
            remote(lt.at[j], lt.at[j], ltsend, ltrecv.at[j], (d, mate)).wait_recv()

    def second(lo, hi, w):
        low = lt[lo:hi].astype(F32).reshape((hi - lo) * 32, 64)
        return jnp.dot(jnp.transpose(low).astype(BF16), w[...], preferred_element_type=F32)

    decay = jnp.exp(-E_HALF * jax.nn.sigmoid(par(7) + second(0, 4, wd2_v)))
    alpha = jax.nn.sigmoid(par(8) + second(4, 8, wa2_v))
    gate = second(8, LOW, wg2_v)
    written = keys * (1.0 + (alpha - 1.0) * par(10))
    rka = removal * alpha
    head_rows(V_D, decay)
    head_rows(V_RKA, rka)
    head_rows(V_W, written)
    head_rows(V_DR, decay * recept)
    readout = (
        state_times(V_DR) - removed * headsum(rka * recept) + values * headsum(written * recept)
    )
    centered = readout - headsum(readout) / 64
    normed = centered * lax.rsqrt(headsum(centered * centered) / 64 + 0.00064) * par(12) + par(13)
    bonus = headsum(recept * written * par(11)) * values
    ap[c] = ((normed + bonus) * gate).astype(BF16)
    k = remote(ap.at[c], ap.at[c], hsem.at[0], hsem.at[1], (d, mate))
    k.start()

    wo_own = wop.at[pl.ds(0, 128), :]
    pltpu.make_async_copy(wo_own, wo_own, psem.at[0]).wait()
    remote(wo_own, wo_own, psem.at[1], psem.at[2], (d, mate)).wait_recv()
    k.wait()

    def scatter(pair, w, send, recv, sem):
        @pl.loop(0, NQ // 2)
        def _(i):
            t = (i + q // 2) % (NQ // 2)
            y = jnp.dot(
                pair, w[:, pl.ds(pl.multiple_of(t * 256, 256), 256)], preferred_element_type=F32
            )
            for u in (0, 1):
                to = 2 * t + u
                block = y[:, 128 * u : 128 * u + 128]
                send[to] = block.astype(BF16)

                @pl.when(to != q)
                def _(to=to):
                    remote(send.at[to], recv.at[q], sem.at[0], sem.at[1], (d, 2 * to + c)).start()

                @pl.when(to == q)
                def _(block=block):
                    zf[...] = block
                    recv[q] = jnp.zeros((64, 128), BF16)

    def arrived(recv, sem):
        part = recv.at[pl.ds(0, NQ - 1)]
        remote(part, part, sem.at[0], sem.at[1], (d, mate)).wait_recv()
        total = zf[...]
        for t in range(NQ):
            total = total + recv[t].astype(F32)
        return total

    scatter(jnp.concatenate([ap[0], ap[1]], axis=1), wop, zs, zr, z1sem)

    @pl.loop(0, 64, unroll=4)
    def _(b):
        for h in (0, 1):
            row = lambda i: vec[i, h, pl.ds(b, 1), 0:64]
            gone = rowsum(jnp.where(eye, row(V_REM), 0.0))
            val = rowsum(jnp.where(eye, row(V_V), 0.0))
            out_s[b, h] = s_v[b, h] * row(V_D) - gone * row(V_RKA) + val * row(V_W)


    f_fwd = gather_finish(fbuf, fsem)
    midway = own_res + arrived(zr, z1sem)
    mbuf[c, q] = midway.astype(BF16)
    gather_start(mbuf, msem)
    f_fwd.wait_recv()
    m_fwd = gather_finish(mbuf, msem)
    m_fwd.wait_recv()

    mean3 = rowsum(over_blocks(lambda cc, t, acc: acc + mbuf[cc, t].astype(F32), zero)) / N
    inv3 = lax.rsqrt(
        rowsum(over_blocks(lambda cc, t, acc: acc + jnp.square(mbuf[cc, t].astype(F32) - mean3), zero)) / N + 1e-05
    )

    def ffn_mixing(cc, t, acc):
        p = params(cc, t)
        base = ((mbuf[cc, t].astype(F32) - mean3) * inv3 * p[10:11] + p[11:12]).astype(BF16).astype(F32)
        mx[0, :, lanes(2 * t + cc)] = (base + (fbuf[cc, t].astype(F32) - base) * p[12:13]).astype(BF16)
        return acc

    over_blocks(ffn_mixing, 0)
    l_up.wait()
    up = jnp.dot(mx[0], wup_v[...], preferred_element_type=F32)
    hp[c] = jnp.square(jnp.maximum(up, 0.0)).astype(BF16)
    k = remote(hp.at[c], hp.at[c], hsem.at[2], hsem.at[3], (d, mate))
    k.start()
    ov_ffn[...] = ((midway - mean3) * inv3 * par(4) + par(5)).astype(BF16)
    wdn_own = wdp.at[pl.ds(0, 512), :]
    pltpu.make_async_copy(wdn_own, wdn_own, psem.at[3]).wait()
    remote(wdn_own, wdn_own, psem.at[4], psem.at[5], (d, mate)).wait_recv()
    k.wait()
    scatter(jnp.concatenate([hp[0], hp[1]], axis=1), wdp, zs2, zr2, z2sem)
    ov_h[...] = midway + arrived(zr2, z2sem)

    part = idv.at[pl.ds(0, ND - 1)]
    remote(part, part, zsem.at[0], zsem.at[1], (d, mate)).wait_send()
    part = rows_s.at[pl.ds(0, ND - 1)]
    remote(part, part, zsem.at[2], zsem.at[3], (d, mate)).wait_send()
    for buf, sem, k in ((abuf, asem, a_fwd), (ebuf, esem, e_fwd), (fbuf, fsem, f_fwd), (mbuf, msem, m_fwd)):
        gather_sent(buf, sem)
        k.wait_send()

    @pl.loop(0, LOW)
    def _(j):
        @pl.when(j != me)
        def _():
            piece = wts.at[pl.ds(0, 32), :]
            remote(piece, piece, wsem.at[j], wrecv, (d, mate)).wait_send()

    @pl.when(me < LOW)
    def _():
        part = lt.at[pl.ds(0, NM - 1)]
        remote(part, part, ltsend, ltrecv.at[0], (d, mate)).wait_send()

    remote(wo_own, wo_own, psem.at[1], psem.at[2], (d, mate)).wait_send()
    remote(wdn_own, wdn_own, psem.at[4], psem.at[5], (d, mate)).wait_send()
    for buf, sem in ((zs, z1sem), (zs2, z2sem)):
        part = buf.at[pl.ds(0, NQ - 1)]
        remote(part, part, sem.at[0], sem.at[1], (d, mate)).wait_send()


def write_out(*refs):
    sem = refs[10]
    copies = [pltpu.make_async_copy(refs[i], refs[5 + i], sem.at[i]) for i in range(5)]
    for k in copies:
        k.start()
    for k in copies:
        k.wait()


def per_device(
    ids, table, g1, b1, g2, b2, prior_rec, lerp, wd1, wd2, fbase, wa1, wa2, abase, wg1, wg2, erase, lcoef, reward,
    wr, wk, wv, state, clg, clb, wo, g3, b3, prior_ffn, lerp_ffn, wup, wdn,
):
    line = lambda x: x.reshape(1, 128)
    vocab = table.shape[0]
    operands = (
        ids.reshape(1, 64), table.reshape(vocab // 8, 8, 128), prior_rec, lerp, wd1, wd2, wa1, wa2, wg1.T, wg2,
        wr, wk, wv, state, wo, prior_ffn, wup, wdn,
        *map(line, (g1, b1, g2, b2, g3, b3, lerp_ffn, fbase, abase, erase, lcoef, reward, clg, clb)),
    )
    vmem = pltpu.VMEM
    dma = pltpu.SemaphoreType.DMA
    scratch = [
        vmem((ND, 1, 64), jnp.int32), pltpu.SMEM((ND, 1, 64), jnp.int32), vmem((vocab // 8, 8, 128), BF16),
        vmem((14, 1, 128), BF16), vmem((6, 128), BF16),
        vmem((128, 128), BF16), vmem((128, 128), BF16), vmem((128, 128), BF16), vmem((128, 128), BF16),
        vmem((480, 128), BF16),
        vmem((N, 128), BF16), vmem((N, 128), BF16), vmem((N, 128), BF16), vmem((64, 2, 64, 64), F32),
        vmem((256, 2048), BF16), vmem((N, 512), BF16), vmem((1024, 2048), BF16),
        vmem((ND, 64, 128), BF16), vmem((ND, 64, 128), BF16),
        vmem((2, NQ, 80, 128), BF16), vmem((2, NQ, 64, 128), BF16), vmem((2, NQ, 64, 128), BF16), vmem((2, NQ, 64, 128), BF16),
        vmem((736, 128), BF16), vmem((32, N), BF16), vmem((4, 64, N), BF16), vmem((2, NQ, 64, 128), F32),
        vmem((NM, 32, 64), BF16), vmem((7, 2, 64, 128), F32), vmem((2, 64, 128), F32),
        vmem((2, 64, 128), BF16), vmem((64, 128), F32),
        vmem((NQ, 64, 128), BF16), vmem((NQ, 64, 128), BF16), vmem((NQ, 64, 128), BF16), vmem((NQ, 64, 128), BF16),
        vmem((2, 64, 512), BF16),
        dma((32,)), dma((4,)), dma((4,)), dma((4,)), dma((4,)), dma((4,)), dma((LOW,)), dma, dma, dma((LOW,)),
        dma((6,)), dma((2,)), dma((2,)), dma((4,)),
    ]
    anywhere = pl.BlockSpec(memory_space=pltpu.HBM)
    inside = pl.BlockSpec(memory_space=pltpu.VMEM)
    shapes = (((64, 128), F32), (state.shape, F32), ((64, 128), BF16), ((64, 128), BF16), ((64, 128), BF16))
    kept = pl.pallas_call(
        whole_step,
        name="whole_step",
        out_shape=tuple(pltpu.VMEM(*x) for x in shapes),
        in_specs=[anywhere] * len(operands),
        out_specs=[inside] * 5,
        scratch_shapes=scratch,
        compiler_params=pltpu.CompilerParams(
            collective_id=0, has_side_effects=True, vmem_limit_bytes=VMEM_GRANT
        ),
    )(*operands)
    return pl.pallas_call(
        write_out,
        name="write_out",
        out_shape=tuple(jax.ShapeDtypeStruct(*x) for x in shapes),
        in_specs=[inside] * 5,
        out_specs=[anywhere] * 5,
        scratch_shapes=[dma((5,))],
        compiler_params=pltpu.CompilerParams(vmem_limit_bytes=1 << 20),
    )(*kept)


def solution(mesh):
    col = P(None, "mp")
    row = P("mp", None)
    one = P("mp")
    both = P("dp", "mp")
    return jax.shard_map(
        per_device,
        mesh=mesh,
        in_specs=(
            P("dp"), both, one, one, one, one, both, col, row, col, one, row, col, one, row, col, one, one, one,
            col, col, col, P("dp", "mp", None, None), one, one, row, one, one, both, one, col, row,
        ),
        out_specs=(both, P("dp", "mp", None, None), both, both, both),
        check_vma=False,
    )
```

```python
import jax
import jax.numpy as jnp
from jax import lax
from jax.experimental import pallas as pl
from jax.experimental.pallas import tpu as pltpu
from jax.sharding import PartitionSpec as P

MESH = pl.DeviceIdType.MESH
F32 = jnp.float32
BF16 = jnp.bfloat16
N = 4096
NQ = 16
NM = 32
ND = 4
LOW = 23
V_RK, V_DR, V_D, V_RKA, V_W, V_V, V_REM = range(7)
VMEM_GRANT = 62_767_104
FAR = sorted(
    ((dy, dx) for dy in range(4) for dx in range(4) if dy or dx),
    key=lambda o: -min(o[0], 4 - o[0]) - min(o[1], 4 - o[1]),
)
E_HALF = 0.6065306597126334


def whole_step(
    ids, table, prior_rec, lerp, wd1, wd2, wa1, wa2, wg1, wg2, wr, wk, wv, state, wo, prior_ffn, wup, wdn,
    g1, b1, g2, b2, g3, b3, lerp_ffn, fbase, abase, erase, lcoef, reward, clg, clb,
    ov_h, out_s, ov_att, ov_ffn, ov_v,
    idv, ids_s, tab, prm, lerp_v, wd1_v, wd2_v, wa1_v, wa2_v, wg2_v, wr_v, wk_v, wv_v, s_v,
    wop, wup_v, wdp, rows_s, rows_r, abuf, ebuf, fbuf, mbuf, wts, wt, mx, res, att, lt, vec, rowb, ap, zf, zs, zr, zs2, zr2, hp,
    ld, zsem, asem, esem, fsem, msem, agot, egot, fgot, mgot, wsem, wrecv, ltsend, ltrecv, psem, z1sem, z2sem, hsem,
):
    d = lax.axis_index("dp")
    me = lax.axis_index("mp")
    q = me // 2
    c = me % 2
    mate = me + 1 - 2 * c

    def remote(src, dst, ssem, rsem, dev):
        return pltpu.make_async_remote_copy(
            src_ref=src, dst_ref=dst, send_sem=ssem, recv_sem=rsem, device_id=dev, device_id_type=MESH
        )

    def lanes(i):
        return pl.ds(pl.multiple_of(i * 128, 128), 128)

    def chip(dy, dx):
        return (q // 4 + dy) % 4 * 4 + (q % 4 + dx) % 4

    barrier = pltpu.get_barrier_semaphore()
    for i in range(1, ND):
        pl.semaphore_signal(barrier, inc=1, device_id=((d + i) % ND, me), device_id_type=MESH)
    for dy, dx in FAR:
        for e in (0, 1):
            pl.semaphore_signal(barrier, inc=1, device_id=(d, 2 * chip(dy, dx) + e), device_id_type=MESH)
    pl.semaphore_signal(barrier, inc=1, device_id=(d, mate), device_id_type=MESH)

    loads = []

    def load(src, dst):
        k = pltpu.make_async_copy(src, dst, ld.at[len(loads)])
        k.start()
        loads.append(k)
        return k

    l_ids = load(ids, idv.at[d])
    l_prm = [
        load(p, prm.at[i])
        for i, p in enumerate((g1, b1, g2, b2, g3, b3, lerp_ffn, fbase, abase, erase, lcoef, reward, clg, clb))
    ]
    l_prm.append(load(lerp, lerp_v))
    l_prior = load(prior_rec, abuf.at[c, q, pl.ds(16, 64), :])
    l_low = [load(wd1, wd1_v), load(wa1, wa1_v), load(wg1, wts.at[pl.ds(256, 480), :])]
    l_tab = load(table, tab)
    l_rkv = [load(wk, wk_v), load(wv, wv_v), load(wr, wr_v)]
    l_s = load(state, s_v)
    l_low2 = [load(wd2, wd2_v), load(wa2, wa2_v), load(wg2, wg2_v)]
    l_priorf = load(prior_ffn, fbuf.at[c, q])

    for k in l_prm:
        k.wait()
    par = lambda i: prm[i].astype(F32)
    lerp_own = lerp_v[...].astype(F32)
    packed = jnp.concatenate(
        [par(0), par(1), par(2), par(3), lerp_own, par(4), par(5), par(6), jnp.zeros((3, 128), F32)], axis=0
    )
    abuf[c, q, 0:16, :] = packed.astype(BF16)
    for k in l_low:
        k.wait()
    wts[0:128, :] = jnp.transpose(wd1_v[...].astype(F32)).astype(BF16)
    wts[128:256, :] = jnp.transpose(wa1_v[...].astype(F32)).astype(BF16)
    l_ids.wait()
    l_prior.wait()

    pl.semaphore_wait(barrier, ND - 1 + NM - 1)

    @pl.loop(1, ND)
    def _(i):
        remote(idv.at[d], idv.at[d], zsem.at[0], zsem.at[1], ((d + i) % ND, me)).start()

    def gather_start(buf, sem, got):
        for dy, dx in FAR:
            remote(buf.at[c, q], buf.at[c, q], sem.at[0], got.at[q], (d, 2 * chip(dy, dx) + 1 - c)).start()
        remote(buf.at[c, q], buf.at[c, q], sem.at[0], got.at[q], (d, mate)).start()

    def gather_pass_on(buf, sem, got):
        for dy, dx in FAR[::-1]:
            t = chip(dy, dx)
            remote(buf.at[1 - c, t], buf.at[1 - c, t], sem.at[0], got.at[t], (d, mate)).wait_recv()
            remote(buf.at[1 - c, t], buf.at[1 - c, t], sem.at[1], sem.at[2], (d, mate)).start()

    def gather_end(buf, sem, got):
        remote(buf.at[1 - c, q], buf.at[1 - c, q], sem.at[0], got.at[q], (d, mate)).wait_recv()
        part = buf.at[0, pl.ds(0, NQ - 1)]
        remote(part, part, sem.at[1], sem.at[2], (d, mate)).wait_recv()

    def gather_sent(buf, sem):
        remote(buf.at[0], buf.at[0], sem.at[0], sem.at[2], (d, mate)).wait_send()
        part = buf.at[0, pl.ds(0, NQ - 1)]
        remote(part, part, sem.at[1], sem.at[2], (d, mate)).wait_send()

    gather_start(abuf, asem, agot)

    @pl.loop(0, LOW)
    def _(j):
        @pl.when(j != me)
        def _():
            remote(
                wts.at[pl.ds(pl.multiple_of(j * 32, 32), 32), :], wt.at[:, lanes(me)], wsem.at[j], wrecv, (d, j)
            ).start()

    @pl.when(me < LOW)
    def _():
        wt[:, lanes(me)] = wts[pl.ds(pl.multiple_of(me * 32, 32), 32), :]

    own_w = []
    for t in range(NQ):
        own_w.append(
            (
                pltpu.make_async_copy(
                    wo.at[:, lanes(2 * t + 1 - c)],
                    wop.at[pl.ds(pl.multiple_of(c * 128, 128), 128), pl.ds(t * 128, 128)],
                    psem.at[0],
                ),
                remote(
                    wo.at[:, lanes(2 * t + c)],
                    wop.at[pl.ds(pl.multiple_of(c * 128, 128), 128), pl.ds(t * 128, 128)],
                    psem.at[1],
                    psem.at[2],
                    (d, mate),
                ),
                pltpu.make_async_copy(
                    wdn.at[:, lanes(2 * t + 1 - c)],
                    wdp.at[pl.ds(pl.multiple_of(c * 512, 512), 512), pl.ds(t * 128, 128)],
                    psem.at[3],
                ),
                remote(
                    wdn.at[:, lanes(2 * t + c)],
                    wdp.at[pl.ds(pl.multiple_of(c * 512, 512), 512), pl.ds(t * 128, 128)],
                    psem.at[4],
                    psem.at[5],
                    (d, mate),
                ),
            )
        )
    for k in own_w:
        k[0].start()
        k[1].start()
    l_up = load(wup, wup_v)
    for k in own_w:
        k[2].start()
        k[3].start()

    part = idv.at[pl.ds(0, ND - 1)]
    remote(part, part, zsem.at[0], zsem.at[1], (d, mate)).wait_recv()
    k = pltpu.make_async_copy(idv, ids_s, ld.at[len(loads)])
    k.start()
    l_tab.wait()
    k.wait()
    bits = (tab.shape[0] * 8).bit_length() - 1
    sub8 = lax.broadcasted_iota(jnp.int32, (8, 128), 0)

    for i in range(ND):
        s = (d + 1 + i) % ND

        @pl.loop(0, 8, unroll=4)
        def _(g, s=s, i=i):
            block = jnp.zeros((8, 128), F32)
            for u in range(8):
                token = ids_s[s, 0, g * 8 + u]
                eight = tab[lax.shift_right_logical(token, 3) & (tab.shape[0] - 1)].astype(F32)
                want = jnp.where(lax.shift_right_logical(token, bits) == d, token & 7, 8)
                row = jnp.sum(jnp.where(sub8 == want, eight, 0.0), axis=0, keepdims=True)
                block = jnp.where(sub8 == u, row, block)
            rowb[i % 2, pl.ds(pl.multiple_of(g * 8, 8), 8), :] = block

        if i < ND - 1:
            rows_s[s] = rowb[i % 2].astype(BF16)
            remote(rows_s.at[s], rows_r.at[d], zsem.at[2], zsem.at[3], (s, me)).start()
        else:
            rows_r[d] = rowb[i % 2].astype(BF16)

    gather_pass_on(abuf, asem, agot)

    part = rows_r.at[pl.ds(0, ND - 1)]
    remote(part, part, zsem.at[2], zsem.at[3], (d, mate)).wait_recv()
    found = rows_r[0].astype(F32)
    for s in range(1, ND):
        found = found + rows_r[s].astype(F32)
    ebuf[c, q] = found.astype(BF16)
    gather_start(ebuf, esem, egot)
    gather_end(abuf, asem, agot)
    l_priorf.wait()
    gather_pass_on(ebuf, esem, egot)
    gather_end(ebuf, esem, egot)

    def params(cc, t):
        return abuf[cc, t, 0:16, :].astype(F32)

    zero = jnp.zeros((64, 128), F32)

    def over_blocks(body, init):
        def step(t, acc):
            for cc in (0, 1):
                acc = body(cc, t, acc)
            return acc

        return lax.fori_loop(0, NQ, step, init)

    def rowsum(x):
        return jnp.sum(x, axis=-1, keepdims=True)

    mean1 = rowsum(over_blocks(lambda cc, t, acc: acc + ebuf[cc, t].astype(F32), zero)) / N
    inv1 = lax.rsqrt(
        rowsum(over_blocks(lambda cc, t, acc: acc + jnp.square(ebuf[cc, t].astype(F32) - mean1), zero)) / N + 1e-05
    )

    def first_norm(cc, t, acc):
        p = params(cc, t)
        r = (ebuf[cc, t].astype(F32) - mean1) * inv1 * p[0:1] + p[1:2]
        res[cc, t] = r
        return acc + r

    mean2 = rowsum(over_blocks(first_norm, zero)) / N
    inv2 = lax.rsqrt(rowsum(over_blocks(lambda cc, t, acc: acc + jnp.square(res[cc, t] - mean2), zero)) / N + 1e-05)

    def mixing(cc, t, acc):
        p = params(cc, t)
        base = ((res[cc, t] - mean2) * inv2 * p[2:3] + p[3:4]).astype(BF16)
        att[cc, t] = base
        base = base.astype(F32)
        low = jnp.where(me < 4, p[5:6], jnp.where(me < 8, p[8:9], p[9:10]))
        mx[0, :, lanes(2 * t + cc)] = (base + (abuf[cc, t, 16:80, :].astype(F32) - base) * low).astype(BF16)
        return acc

    over_blocks(mixing, 0)
    own_res = res[c, q]

    @pl.when(me < LOW)
    def _():
        got = wt.at[:, pl.ds(0, (NM - 1) * 128)]
        remote(got, got, wsem.at[0], wrecv, (d, mate)).wait_recv()
        low = lax.dot_general(wt[...], mx[0], (((1,), (1,)), ((), ())), preferred_element_type=F32)
        low = jnp.where(me < 4, jnp.tanh(low), jnp.where(me < 8, low, jax.nn.sigmoid(low)))
        lt[me] = jnp.concatenate([low[0:16], low[16:32]], axis=1).astype(BF16)
        for dy, dx in FAR:
            for e in (0, 1):
                remote(lt.at[me], lt.at[me], ltsend, ltrecv.at[me], (d, 2 * chip(dy, dx) + e)).start()
        remote(lt.at[me], lt.at[me], ltsend, ltrecv.at[me], (d, mate)).start()

    gather_start(fbuf, fsem, fgot)

    def mixing_rest(cc, t, acc):
        p = params(cc, t)
        base = att[cc, t].astype(F32)
        delta = abuf[cc, t, 16:80, :].astype(F32) - base
        at = lanes(2 * t + cc)
        mx[1, :, at] = (base + delta * p[6:7]).astype(BF16)
        mx[2, :, at] = (base + delta * p[7:8]).astype(BF16)
        mx[3, :, at] = (base + delta * p[4:5]).astype(BF16)
        return acc

    over_blocks(mixing_rest, 0)
    ov_att[...] = att[c, q]

    def head_rows(i, x):
        vec[i, 0] = x
        vec[i, 1] = pltpu.roll(x, 64, axis=1)

    left = lax.broadcasted_iota(jnp.int32, (64, 128), 1) < 64
    eye = lax.broadcasted_iota(jnp.int32, (64, 64), 0) == lax.broadcasted_iota(jnp.int32, (64, 64), 1)

    def headsum(x):
        return jnp.where(left, rowsum(jnp.where(left, x, 0.0)), rowsum(jnp.where(left, 0.0, x)))

    def projected(i, w, k):
        k.wait()
        return jnp.dot(mx[i], w[...], preferred_element_type=F32)

    def state_times(i):
        @pl.loop(0, 64, unroll=8)
        def _(b):
            for h in (0, 1):
                col = rowsum(s_v[b, h] * vec[i, h, pl.ds(b, 1), 0:64])
                rowb[h, pl.ds(b, 1), 0:64] = jnp.sum(jnp.where(eye, col, 0.0), axis=0, keepdims=True)

        return jnp.where(left, rowb[0], pltpu.roll(rowb[1], 64, axis=1))

    keys = projected(1, wk_v, l_rkv[0])
    removal = keys * par(9)
    removal = removal * lax.rsqrt(headsum(removal * removal) + 1e-06)
    values = projected(2, wv_v, l_rkv[1])
    recept = projected(3, wr_v, l_rkv[2])
    ov_v[...] = values.astype(BF16)
    head_rows(V_RK, removal)
    head_rows(V_V, values)
    rowb[0] = zero
    rowb[1] = zero
    l_s.wait()
    removed = state_times(V_RK)
    head_rows(V_REM, removed)

    for k in l_low2:
        k.wait()

    @pl.loop(0, LOW)
    def _(j):
        @pl.when(j != me)
        def _():
            remote(lt.at[j], lt.at[j], ltsend, ltrecv.at[j], (d, mate)).wait_recv()

    def second(lo, hi, w):
        n = hi - lo
        low = jnp.transpose(lt[lo:hi].astype(F32).reshape(n * 16, 128)).astype(BF16)
        parts = [jnp.concatenate([w[32 * j + 16 * u : 32 * j + 16 * u + 16, :] for j in range(n)], axis=0) for u in (0, 1)]
        return jnp.dot(low[0:64], parts[0], preferred_element_type=F32) + jnp.dot(
            low[64:128], parts[1], preferred_element_type=F32
        )

    decay = jnp.exp(-E_HALF * jax.nn.sigmoid(par(7) + second(0, 4, wd2_v)))
    alpha = jax.nn.sigmoid(par(8) + second(4, 8, wa2_v))
    gate = second(8, LOW, wg2_v)
    written = keys * (1.0 + (alpha - 1.0) * par(10))
    rka = removal * alpha
    head_rows(V_D, decay)
    head_rows(V_RKA, rka)
    head_rows(V_W, written)
    head_rows(V_DR, decay * recept)
    readout = (
        state_times(V_DR) - removed * headsum(rka * recept) + values * headsum(written * recept)
    )
    centered = readout - headsum(readout) / 64
    normed = centered * lax.rsqrt(headsum(centered * centered) / 64 + 0.00064) * par(12) + par(13)
    bonus = headsum(recept * written * par(11)) * values
    ap[c] = ((normed + bonus) * gate).astype(BF16)
    k = remote(ap.at[c], ap.at[c], hsem.at[0], hsem.at[1], (d, mate))
    k.start()

    wo_own = wop.at[pl.ds(0, 128), :]
    pltpu.make_async_copy(wo_own, wo_own, psem.at[0]).wait()
    remote(wo_own, wo_own, psem.at[1], psem.at[2], (d, mate)).wait_recv()
    def scatter(own, pair, w, width, send, recv, sem, k):
        rows_own = pl.ds(pl.multiple_of(c * width, width), width)
        rows_mate = pl.ds(pl.multiple_of((1 - c) * width, width), width)
        chunks = [(dy, dx) for dy in (2, 1, 3, 0) for dx in (1, 0)]
        place = [(q // 4 + dy) % 4 * 2 + (q % 4 // 2 + dx) % 2 for dy, dx in chunks]
        cols = [pl.ds(pl.multiple_of(t * 256, 256), 256) for t in place]
        for i in range(8):
            zf[i] = jnp.dot(own, w[rows_own, cols[i]], preferred_element_type=F32)
        k.wait()
        other = pair[1 - c]
        for i in range(8):
            y = zf[i] + jnp.dot(other, w[rows_mate, cols[i]], preferred_element_type=F32)
            for u in (0, 1):
                to = 2 * place[i] + u
                send[to] = y[:, 128 * u : 128 * u + 128].astype(BF16)
                remote(send.at[to], recv.at[q], sem.at[0], sem.at[1], (d, 2 * to + 1 - c)).start()

    def arrived(recv, sem):
        remote(recv, recv, sem.at[0], sem.at[1], (d, mate)).wait_recv()
        total = recv[0].astype(F32)
        for t in range(1, NQ):
            total = total + recv[t].astype(F32)
        return total

    scatter(ap[c], ap, wop, 128, zs, zr, z1sem, k)

    @pl.loop(0, 64, unroll=4)
    def _(b):
        for h in (0, 1):
            row = lambda i: vec[i, h, pl.ds(b, 1), 0:64]
            gone = rowsum(jnp.where(eye, row(V_REM), 0.0))
            val = rowsum(jnp.where(eye, row(V_V), 0.0))
            out_s[b, h] = s_v[b, h] * row(V_D) - gone * row(V_RKA) + val * row(V_W)


    gather_pass_on(fbuf, fsem, fgot)
    midway = own_res + arrived(zr, z1sem)
    mbuf[c, q] = midway.astype(BF16)
    gather_start(mbuf, msem, mgot)
    gather_end(fbuf, fsem, fgot)
    gather_pass_on(mbuf, msem, mgot)
    gather_end(mbuf, msem, mgot)

    mean3 = rowsum(over_blocks(lambda cc, t, acc: acc + mbuf[cc, t].astype(F32), zero)) / N
    inv3 = lax.rsqrt(
        rowsum(over_blocks(lambda cc, t, acc: acc + jnp.square(mbuf[cc, t].astype(F32) - mean3), zero)) / N + 1e-05
    )

    def ffn_mixing(cc, t, acc):
        p = params(cc, t)
        base = ((mbuf[cc, t].astype(F32) - mean3) * inv3 * p[10:11] + p[11:12]).astype(BF16).astype(F32)
        mx[0, :, lanes(2 * t + cc)] = (base + (fbuf[cc, t].astype(F32) - base) * p[12:13]).astype(BF16)
        return acc

    over_blocks(ffn_mixing, 0)
    l_up.wait()
    up = jnp.dot(mx[0], wup_v[...], preferred_element_type=F32)
    hp[c] = jnp.square(jnp.maximum(up, 0.0)).astype(BF16)
    k = remote(hp.at[c], hp.at[c], hsem.at[2], hsem.at[3], (d, mate))
    k.start()
    ov_ffn[...] = ((midway - mean3) * inv3 * par(4) + par(5)).astype(BF16)
    wdn_own = wdp.at[pl.ds(0, 512), :]
    pltpu.make_async_copy(wdn_own, wdn_own, psem.at[3]).wait()
    remote(wdn_own, wdn_own, psem.at[4], psem.at[5], (d, mate)).wait_recv()
    scatter(hp[c], hp, wdp, 512, zs2, zr2, z2sem, k)
    ov_h[...] = midway + arrived(zr2, z2sem)

    part = idv.at[pl.ds(0, ND - 1)]
    remote(part, part, zsem.at[0], zsem.at[1], (d, mate)).wait_send()
    part = rows_s.at[pl.ds(0, ND - 1)]
    remote(part, part, zsem.at[2], zsem.at[3], (d, mate)).wait_send()
    for buf, sem in ((abuf, asem), (ebuf, esem), (fbuf, fsem), (mbuf, msem)):
        gather_sent(buf, sem)

    @pl.loop(0, LOW)
    def _(j):
        @pl.when(j != me)
        def _():
            piece = wts.at[pl.ds(0, 32), :]
            remote(piece, piece, wsem.at[j], wrecv, (d, mate)).wait_send()

    @pl.when(me < LOW)
    def _():
        part = lt.at[pl.ds(0, NM - 1)]
        remote(part, part, ltsend, ltrecv.at[0], (d, mate)).wait_send()

    remote(wo_own, wo_own, psem.at[1], psem.at[2], (d, mate)).wait_send()
    remote(wdn_own, wdn_own, psem.at[4], psem.at[5], (d, mate)).wait_send()
    for buf, sem in ((zs, z1sem), (zs2, z2sem)):
        remote(buf, buf, sem.at[0], sem.at[1], (d, mate)).wait_send()


def write_out(*refs):
    sem = refs[10]
    copies = [pltpu.make_async_copy(refs[i], refs[5 + i], sem.at[i]) for i in range(5)]
    for k in copies:
        k.start()
    for k in copies:
        k.wait()


def per_device(
    ids, table, g1, b1, g2, b2, prior_rec, lerp, wd1, wd2, fbase, wa1, wa2, abase, wg1, wg2, erase, lcoef, reward,
    wr, wk, wv, state, clg, clb, wo, g3, b3, prior_ffn, lerp_ffn, wup, wdn,
):
    line = lambda x: x.reshape(1, 128)
    vocab = table.shape[0]
    operands = (
        ids.reshape(1, 64), table.reshape(vocab // 8, 8, 128), prior_rec, lerp, wd1, wd2, wa1, wa2, wg1.T, wg2,
        wr, wk, wv, state, wo, prior_ffn, wup, wdn,
        *map(line, (g1, b1, g2, b2, g3, b3, lerp_ffn, fbase, abase, erase, lcoef, reward, clg, clb)),
    )
    vmem = pltpu.VMEM
    dma = pltpu.SemaphoreType.DMA
    scratch = [
        vmem((ND, 1, 64), jnp.int32), pltpu.SMEM((ND, 1, 64), jnp.int32), vmem((vocab // 8, 8, 128), BF16),
        vmem((14, 1, 128), BF16), vmem((6, 128), BF16),
        vmem((128, 128), BF16), vmem((128, 128), BF16), vmem((128, 128), BF16), vmem((128, 128), BF16),
        vmem((480, 128), BF16),
        vmem((N, 128), BF16), vmem((N, 128), BF16), vmem((N, 128), BF16), vmem((64, 2, 64, 64), F32),
        vmem((256, 2048), BF16), vmem((N, 512), BF16), vmem((1024, 2048), BF16),
        vmem((ND, 64, 128), BF16), vmem((ND, 64, 128), BF16),
        vmem((2, NQ, 80, 128), BF16), vmem((2, NQ, 64, 128), BF16), vmem((2, NQ, 64, 128), BF16), vmem((2, NQ, 64, 128), BF16),
        vmem((736, 128), BF16), vmem((32, N), BF16), vmem((4, 64, N), BF16), vmem((2, NQ, 64, 128), F32),
        vmem((2, NQ, 64, 128), BF16), vmem((NM, 16, 128), BF16), vmem((7, 2, 64, 128), F32), vmem((2, 64, 128), F32),
        vmem((2, 64, 128), BF16), vmem((8, 64, 256), F32),
        vmem((NQ, 64, 128), BF16), vmem((NQ, 64, 128), BF16), vmem((NQ, 64, 128), BF16), vmem((NQ, 64, 128), BF16),
        vmem((2, 64, 512), BF16),
        dma((32,)), dma((4,)), dma((3,)), dma((3,)), dma((3,)), dma((3,)), dma((NQ,)), dma((NQ,)), dma((NQ,)), dma((NQ,)), dma((LOW,)), dma, dma, dma((LOW,)),
        dma((6,)), dma((2,)), dma((2,)), dma((4,)),
    ]
    anywhere = pl.BlockSpec(memory_space=pltpu.HBM)
    inside = pl.BlockSpec(memory_space=pltpu.VMEM)
    shapes = (((64, 128), F32), (state.shape, F32), ((64, 128), BF16), ((64, 128), BF16), ((64, 128), BF16))
    kept = pl.pallas_call(
        whole_step,
        name="whole_step",
        out_shape=tuple(pltpu.VMEM(*x) for x in shapes),
        in_specs=[anywhere] * len(operands),
        out_specs=[inside] * 5,
        scratch_shapes=scratch,
        compiler_params=pltpu.CompilerParams(
            collective_id=0, has_side_effects=True, vmem_limit_bytes=VMEM_GRANT
        ),
    )(*operands)
    return pl.pallas_call(
        write_out,
        name="write_out",
        out_shape=tuple(jax.ShapeDtypeStruct(*x) for x in shapes),
        in_specs=[inside] * 5,
        out_specs=[anywhere] * 5,
        scratch_shapes=[dma((5,))],
        compiler_params=pltpu.CompilerParams(vmem_limit_bytes=1 << 20),
    )(*kept)


def solution(mesh):
    col = P(None, "mp")
    row = P("mp", None)
    one = P("mp")
    both = P("dp", "mp")
    return jax.shard_map(
        per_device,
        mesh=mesh,
        in_specs=(
            P("dp"), both, one, one, one, one, both, col, row, col, one, row, col, one, row, col, one, one, one,
            col, col, col, P("dp", "mp", None, None), one, one, row, one, one, both, one, col, row,
        ),
        out_specs=(both, P("dp", "mp", None, None), both, both, both),
        check_vma=False,
    )
```

```python
import jax
import jax.numpy as jnp
from jax import lax
from jax.experimental import pallas as pl
from jax.experimental.pallas import tpu as pltpu
from jax.sharding import PartitionSpec as P

MESH = pl.DeviceIdType.MESH
F32 = jnp.float32
BF16 = jnp.bfloat16
N = 4096
NQ = 16
NM = 32
ND = 4
LOW = 23
V_D, V_RKA, V_W, V_V, V_REM = range(5)
VMEM_GRANT = 62_767_104
FAR = sorted(
    ((dy, dx) for dy in range(4) for dx in range(4) if dy or dx),
    key=lambda o: -min(o[0], 4 - o[0]) - min(o[1], 4 - o[1]),
)
E_HALF = 0.6065306597126334


def whole_step(
    ids, table, prior_rec, lerp, wd1, wd2, wa1, wa2, wg1, wg2, wr, wk, wv, state, wo, prior_ffn, wup, wdn,
    g1, b1, g2, b2, g3, b3, lerp_ffn, fbase, abase, erase, lcoef, reward, clg, clb,
    ov_h, out_s, ov_att, ov_ffn, ov_v,
    idv, ids_s, tab, prm, lerp_v, wd1_v, wd2_v, wa1_v, wa2_v, wg2_v, wr_v, wk_v, wv_v, s_v,
    wop, wup_v, wdp, si, st, rows_s, rows_r, abuf, ebuf, fbuf, mbuf, wts, wt, mx, res, att, lt, vec, rowb, ap, zf, zs, zr, zs2, zr2, hp,
    ld, zsem, asem, esem, fsem, msem, agot, egot, fgot, mgot, wsem, wrecv, ltsend, ltrecv, psem, z1sem, z2sem, hsem,
):
    d = lax.axis_index("dp")
    me = lax.axis_index("mp")
    q = me // 2
    c = me % 2
    mate = me + 1 - 2 * c

    def remote(src, dst, ssem, rsem, dev):
        return pltpu.make_async_remote_copy(
            src_ref=src, dst_ref=dst, send_sem=ssem, recv_sem=rsem, device_id=dev, device_id_type=MESH
        )

    def lanes(i):
        return pl.ds(pl.multiple_of(i * 128, 128), 128)

    def chip(dy, dx):
        return (q // 4 + dy) % 4 * 4 + (q % 4 + dx) % 4

    barrier = pltpu.get_barrier_semaphore()
    for i in range(1, ND):
        for m in (me, mate):
            pl.semaphore_signal(barrier, inc=1, device_id=((d + i) % ND, m), device_id_type=MESH)
    for dy, dx in FAR:
        for e in (0, 1):
            pl.semaphore_signal(barrier, inc=1, device_id=(d, 2 * chip(dy, dx) + e), device_id_type=MESH)
    pl.semaphore_signal(barrier, inc=1, device_id=(d, mate), device_id_type=MESH)

    loads = []

    def load(src, dst):
        k = pltpu.make_async_copy(src, dst, ld.at[len(loads)])
        k.start()
        loads.append(k)
        return k

    l_ids = load(ids, idv.at[d])
    l_prm = [
        load(p, prm.at[i])
        for i, p in enumerate((g1, b1, g2, b2, g3, b3, lerp_ffn, fbase, abase, erase, lcoef, reward, clg, clb))
    ]
    l_prm.append(load(lerp, lerp_v))
    l_prior = load(prior_rec, abuf.at[c, q, pl.ds(16, 64), :])
    l_low = [load(wd1, wd1_v), load(wa1, wa1_v), load(wg1, wts.at[pl.ds(256, 480), :])]
    l_tab = load(table, tab)
    l_low2 = [load(wd2, wd2_v), load(wa2, wa2_v), load(wg2, wg2_v)]
    l_priorf = load(prior_ffn, fbuf.at[c, q])

    for k in l_prm:
        k.wait()
    par = lambda i: prm[i].astype(F32)
    lerp_own = lerp_v[...].astype(F32)
    packed = jnp.concatenate(
        [par(0), par(1), par(2), par(3), lerp_own, par(4), par(5), par(6), jnp.zeros((3, 128), F32)], axis=0
    )
    abuf[c, q, 0:16, :] = packed.astype(BF16)
    for k in l_low:
        k.wait()
    wts[0:128, :] = jnp.transpose(wd1_v[...].astype(F32)).astype(BF16)
    wts[128:256, :] = jnp.transpose(wa1_v[...].astype(F32)).astype(BF16)
    @pl.loop(0, 64)
    def _(i):
        for h in (0, 1):
            pltpu.make_async_copy(state.at[:, h, i, :], si.at[i, h], psem.at[6]).start()

    l_rkv = [load(wk, wk_v), load(wv, wv_v), load(wr, wr_v)]
    l_ids.wait()
    l_prior.wait()

    pl.semaphore_wait(barrier, 2 * (ND - 1) + NM - 1)

    for i in (2, 1, 3):
        remote(idv.at[d], idv.at[d], zsem.at[0], zsem.at[1], ((d + i) % ND, mate)).start()

    def gather_start(buf, sem, got):
        for dy, dx in FAR:
            remote(buf.at[c, q], buf.at[c, q], sem.at[0], got.at[q], (d, 2 * chip(dy, dx) + 1 - c)).start()
        remote(buf.at[c, q], buf.at[c, q], sem.at[0], got.at[q], (d, mate)).start()

    def gather_pass_on(buf, sem, got, use=None, acc=None):
        for dy, dx in FAR[::-1]:
            t = chip(dy, dx)
            remote(buf.at[1 - c, t], buf.at[1 - c, t], sem.at[0], got.at[t], (d, mate)).wait_recv()
            remote(buf.at[1 - c, t], buf.at[1 - c, t], sem.at[1], sem.at[2], (d, mate)).start()
            if use is not None:
                acc = use(1 - c, t, acc)
        return acc

    def gather_end(buf, sem, got):
        remote(buf.at[1 - c, q], buf.at[1 - c, q], sem.at[0], got.at[q], (d, mate)).wait_recv()
        part = buf.at[0, pl.ds(0, NQ - 1)]
        remote(part, part, sem.at[1], sem.at[2], (d, mate)).wait_recv()

    def gather_sent(buf, sem):
        remote(buf.at[0], buf.at[0], sem.at[0], sem.at[2], (d, mate)).wait_send()
        part = buf.at[0, pl.ds(0, NQ - 1)]
        remote(part, part, sem.at[1], sem.at[2], (d, mate)).wait_send()

    gather_start(abuf, asem, agot)

    @pl.loop(0, LOW)
    def _(j):
        @pl.when(j != me)
        def _():
            remote(
                wts.at[pl.ds(pl.multiple_of(j * 32, 32), 32), :], wt.at[:, lanes(me)], wsem.at[j], wrecv, (d, j)
            ).start()

    @pl.when(me < LOW)
    def _():
        wt[:, lanes(me)] = wts[pl.ds(pl.multiple_of(me * 32, 32), 32), :]

    own_w = []
    for t in range(NQ):
        own_w.append(
            (
                pltpu.make_async_copy(
                    wo.at[:, lanes(2 * t + 1 - c)],
                    wop.at[pl.ds(pl.multiple_of(c * 128, 128), 128), pl.ds(t * 128, 128)],
                    psem.at[0],
                ),
                remote(
                    wo.at[:, lanes(2 * t + c)],
                    wop.at[pl.ds(pl.multiple_of(c * 128, 128), 128), pl.ds(t * 128, 128)],
                    psem.at[1],
                    psem.at[2],
                    (d, mate),
                ),
                pltpu.make_async_copy(
                    wdn.at[:, lanes(2 * t + 1 - c)],
                    wdp.at[pl.ds(pl.multiple_of(c * 512, 512), 512), pl.ds(t * 128, 128)],
                    psem.at[3],
                ),
                remote(
                    wdn.at[:, lanes(2 * t + c)],
                    wdp.at[pl.ds(pl.multiple_of(c * 512, 512), 512), pl.ds(t * 128, 128)],
                    psem.at[4],
                    psem.at[5],
                    (d, mate),
                ),
            )
        )
    for k in own_w:
        k[0].start()
        k[1].start()
    l_s = load(state, s_v)
    l_up = load(wup, wup_v)
    for k in own_w:
        k[2].start()
        k[3].start()

    part = idv.at[pl.ds(0, ND - 1)]
    remote(part, part, zsem.at[0], zsem.at[1], (d, mate)).wait_recv()
    k = pltpu.make_async_copy(idv, ids_s, ld.at[len(loads)])
    k.start()
    l_tab.wait()
    k.wait()
    bits = (tab.shape[0] * 8).bit_length() - 1
    sub8 = lax.broadcasted_iota(jnp.int32, (8, 128), 0)

    for i in range(ND):
        s = (d + (2, 1, 3, 0)[i]) % ND

        @pl.loop(0, 8, unroll=4)
        def _(g, s=s, i=i):
            block = jnp.zeros((8, 128), F32)
            for u in range(8):
                token = ids_s[s, 0, g * 8 + u]
                eight = tab[lax.shift_right_logical(token, 3) & (tab.shape[0] - 1)].astype(F32)
                want = jnp.where(lax.shift_right_logical(token, bits) == d, token & 7, 8)
                row = jnp.sum(jnp.where(sub8 == want, eight, 0.0), axis=0, keepdims=True)
                block = jnp.where(sub8 == u, row, block)
            rowb[i % 2, pl.ds(pl.multiple_of(g * 8, 8), 8), :] = block

        if i < ND - 1:
            rows_s[s] = rowb[i % 2].astype(BF16)
            remote(rows_s.at[s], rows_r.at[d], zsem.at[2], zsem.at[3], (s, me)).start()
        else:
            rows_r[d] = rowb[i % 2].astype(BF16)


    part = rows_r.at[pl.ds(0, ND - 1)]
    remote(part, part, zsem.at[2], zsem.at[3], (d, mate)).wait_recv()
    found = rows_r[0].astype(F32)
    for s in range(1, ND):
        found = found + rows_r[s].astype(F32)
    ebuf[c, q] = found.astype(BF16)
    gather_start(ebuf, esem, egot)
    gather_pass_on(abuf, asem, agot)
    gather_end(abuf, asem, agot)
    l_priorf.wait()
    def rowsum(x):
        return jnp.sum(x, axis=-1, keepdims=True)

    zero = jnp.zeros((64, 128), F32)

    def moments_of(buf):
        pivot = rowsum(buf[c, q].astype(F32)) / 128

        def add(cc, t, acc):
            x = buf[cc, t].astype(F32) - pivot
            return acc[0] + x, acc[1] + x * x

        return pivot, add

    def mean_and_scale(pivot, acc):
        shift = rowsum(acc[0]) / N
        return pivot + shift, lax.rsqrt(jnp.maximum(rowsum(acc[1]) / N - shift * shift, 0.0) + 1e-05)

    def gathered_norm(buf, sem, got):
        pivot, add = moments_of(buf)
        acc = gather_pass_on(buf, sem, got, add, (zero, zero))
        gather_end(buf, sem, got)
        acc = add(1 - c, q, acc)
        acc = lax.fori_loop(0, NQ, lambda t, acc: add(c, t, acc), acc, unroll=4)
        return mean_and_scale(pivot, acc)

    mean1, inv1 = gathered_norm(ebuf, esem, egot)

    def params(cc, t):
        return abuf[cc, t, 0:16, :].astype(F32)

    def over_blocks(body, init):
        def step(t, acc):
            for cc in (0, 1):
                acc = body(cc, t, acc)
            return acc

        return lax.fori_loop(0, NQ, step, init)

    own_p = params(c, q)
    own_res = (ebuf[c, q].astype(F32) - mean1) * inv1 * own_p[0:1] + own_p[1:2]
    pivot2 = rowsum(own_res) / 128

    def first_norm(cc, t, acc):
        p = params(cc, t)
        r = (ebuf[cc, t].astype(F32) - mean1) * inv1 * p[0:1] + p[1:2]
        res[cc, t] = r
        r = r - pivot2
        return acc[0] + r, acc[1] + r * r

    mean2, inv2 = mean_and_scale(pivot2, over_blocks(first_norm, (zero, zero)))

    @pl.when(me < LOW)
    def _():
        got = wt.at[:, pl.ds(0, (NM - 1) * 128)]
        remote(got, got, wsem.at[0], wrecv, (d, mate)).wait_recv()

    def mixing(cc, t):
        p = params(cc, t)
        base = ((res[cc, t] - mean2) * inv2 * p[2:3] + p[3:4]).astype(BF16)
        att[cc, t] = base
        base = base.astype(F32)
        rate = jnp.where(me < 4, p[5:6], jnp.where(me < 8, p[8:9], p[9:10]))
        return (base + (abuf[cc, t, 16:80, :].astype(F32) - base) * rate).astype(BF16)

    low = 0.0
    for t in range(NQ):
        x = jnp.concatenate([mixing(0, t), mixing(1, t)], axis=1)
        low = low + lax.dot_general(
            wt[:, 256 * t : 256 * t + 256], x, (((1,), (1,)), ((), ())), preferred_element_type=F32
        )
    low = jnp.where(me < 4, jnp.tanh(low), jnp.where(me < 8, low, jax.nn.sigmoid(low)))

    @pl.when(me < LOW)
    def _():
        lt[me] = jnp.concatenate([low[0:16], low[16:32]], axis=1).astype(BF16)
        for dy, dx in FAR:
            for e in (0, 1):
                remote(lt.at[me], lt.at[me], ltsend, ltrecv.at[me], (d, 2 * chip(dy, dx) + e)).start()
        remote(lt.at[me], lt.at[me], ltsend, ltrecv.at[me], (d, mate)).start()

    gather_start(fbuf, fsem, fgot)

    def mixing_rest(cc, t, acc):
        p = params(cc, t)
        base = att[cc, t].astype(F32)
        delta = abuf[cc, t, 16:80, :].astype(F32) - base
        at = lanes(2 * t + cc)
        mx[1, :, at] = (base + delta * p[6:7]).astype(BF16)
        mx[2, :, at] = (base + delta * p[7:8]).astype(BF16)
        mx[3, :, at] = (base + delta * p[4:5]).astype(BF16)
        return acc

    over_blocks(mixing_rest, 0)
    ov_att[...] = att[c, q]

    def head_rows(i, x):
        vec[i, 0] = x
        vec[i, 1] = pltpu.roll(x, 64, axis=1)

    left = lax.broadcasted_iota(jnp.int32, (64, 128), 1) < 64
    eye = lax.broadcasted_iota(jnp.int32, (64, 64), 0) == lax.broadcasted_iota(jnp.int32, (64, 64), 1)

    def headsum(x):
        return jnp.where(left, rowsum(jnp.where(left, x, 0.0)), rowsum(jnp.where(left, 0.0, x)))

    def projected(i, w, k):
        k.wait()
        return jnp.dot(mx[i], w[...], preferred_element_type=F32)

    def turned(x):
        y = jnp.transpose(x)
        return jnp.concatenate([y[0:64], y[64:128]], axis=1)

    def state_times(x):
        y = turned(x)

        @pl.loop(0, 64, unroll=8)
        def _(i):
            rowb[0, pl.ds(i, 1), :] = jnp.sum(st[i] * y, axis=0, keepdims=True)

        return turned(rowb[0])

    keys = projected(1, wk_v, l_rkv[0])
    removal = keys * par(9)
    removal = removal * lax.rsqrt(headsum(removal * removal) + 1e-06)
    values = projected(2, wv_v, l_rkv[1])
    recept = projected(3, wr_v, l_rkv[2])
    ov_v[...] = values.astype(BF16)
    head_rows(V_V, values)
    pltpu.make_async_copy(si, si, psem.at[6]).wait()

    @pl.loop(0, 64, unroll=4)
    def _(i):
        st[i] = jnp.transpose(si[i].reshape(128, 64))

    removed = state_times(removal)
    head_rows(V_REM, removed)

    for k in l_low2:
        k.wait()

    @pl.loop(0, LOW)
    def _(j):
        @pl.when(j != me)
        def _():
            remote(lt.at[j], lt.at[j], ltsend, ltrecv.at[j], (d, mate)).wait_recv()

    def second(lo, hi, w):
        n = hi - lo
        low = jnp.transpose(lt[lo:hi].astype(F32).reshape(n * 16, 128)).astype(BF16)
        parts = [jnp.concatenate([w[32 * j + 16 * u : 32 * j + 16 * u + 16, :] for j in range(n)], axis=0) for u in (0, 1)]
        return jnp.dot(low[0:64], parts[0], preferred_element_type=F32) + jnp.dot(
            low[64:128], parts[1], preferred_element_type=F32
        )

    decay = jnp.exp(-E_HALF * jax.nn.sigmoid(par(7) + second(0, 4, wd2_v)))
    alpha = jax.nn.sigmoid(par(8) + second(4, 8, wa2_v))
    gate = second(8, LOW, wg2_v)
    written = keys * (1.0 + (alpha - 1.0) * par(10))
    rka = removal * alpha
    head_rows(V_D, decay)
    head_rows(V_RKA, rka)
    head_rows(V_W, written)
    readout = (
        state_times(decay * recept) - removed * headsum(rka * recept) + values * headsum(written * recept)
    )
    centered = readout - headsum(readout) / 64
    normed = centered * lax.rsqrt(headsum(centered * centered) / 64 + 0.00064) * par(12) + par(13)
    bonus = headsum(recept * written * par(11)) * values
    ap[c] = ((normed + bonus) * gate).astype(BF16)
    k = remote(ap.at[c], ap.at[c], hsem.at[0], hsem.at[1], (d, mate))
    k.start()

    wo_own = wop.at[pl.ds(0, 128), :]
    pltpu.make_async_copy(wo_own, wo_own, psem.at[0]).wait()
    remote(wo_own, wo_own, psem.at[1], psem.at[2], (d, mate)).wait_recv()
    def scatter(own, pair, w, width, send, recv, sem, k):
        rows_own = pl.ds(pl.multiple_of(c * width, width), width)
        rows_mate = pl.ds(pl.multiple_of((1 - c) * width, width), width)
        rows = [(q // 4 + dy) % 4 for dy in (2, 1, 3, 0)]
        cols = [pl.ds(pl.multiple_of(t * 512, 512), 512) for t in rows]
        for i in range(4):
            zf[i] = jnp.dot(own, w[rows_own, cols[i]], preferred_element_type=F32)
        k.wait()
        other = pair[1 - c]
        for i in range(4):
            y = zf[i] + jnp.dot(other, w[rows_mate, cols[i]], preferred_element_type=F32)
            for u in range(4):
                to = 4 * rows[i] + u
                send[to] = y[:, 128 * u : 128 * u + 128].astype(BF16)
            for u in range(4):
                to = 4 * rows[i] + u
                remote(send.at[to], recv.at[q], sem.at[0], sem.at[1], (d, 2 * to + 1 - c)).start()

    def arrived(recv, sem):
        remote(recv, recv, sem.at[0], sem.at[1], (d, mate)).wait_recv()
        total = recv[0].astype(F32)
        for t in range(1, NQ):
            total = total + recv[t].astype(F32)
        return total

    scatter(ap[c], ap, wop, 128, zs, zr, z1sem, k)

    l_s.wait()

    @pl.loop(0, 64, unroll=4)
    def _(b):
        for h in (0, 1):
            row = lambda i: vec[i, h, pl.ds(b, 1), 0:64]
            gone = rowsum(jnp.where(eye, row(V_REM), 0.0))
            val = rowsum(jnp.where(eye, row(V_V), 0.0))
            out_s[b, h] = s_v[b, h] * row(V_D) - gone * row(V_RKA) + val * row(V_W)


    gather_pass_on(fbuf, fsem, fgot)
    midway = own_res + arrived(zr, z1sem)
    mbuf[c, q] = midway.astype(BF16)
    gather_start(mbuf, msem, mgot)
    gather_end(fbuf, fsem, fgot)
    mean3, inv3 = gathered_norm(mbuf, msem, mgot)

    def ffn_mixed(cc, t):
        p = params(cc, t)
        base = ((mbuf[cc, t].astype(F32) - mean3) * inv3 * p[10:11] + p[11:12]).astype(BF16).astype(F32)
        return (base + (fbuf[cc, t].astype(F32) - base) * p[12:13]).astype(BF16)

    l_up.wait()
    up = 0.0
    for t in range(NQ):
        x = jnp.concatenate([ffn_mixed(0, t), ffn_mixed(1, t)], axis=1)
        up = up + jnp.dot(x, wup_v[256 * t : 256 * t + 256, :], preferred_element_type=F32)
    hp[c] = jnp.square(jnp.maximum(up, 0.0)).astype(BF16)
    k = remote(hp.at[c], hp.at[c], hsem.at[2], hsem.at[3], (d, mate))
    k.start()
    ov_ffn[...] = ((midway - mean3) * inv3 * par(4) + par(5)).astype(BF16)
    wdn_own = wdp.at[pl.ds(0, 512), :]
    pltpu.make_async_copy(wdn_own, wdn_own, psem.at[3]).wait()
    remote(wdn_own, wdn_own, psem.at[4], psem.at[5], (d, mate)).wait_recv()
    scatter(hp[c], hp, wdp, 512, zs2, zr2, z2sem, k)
    ov_h[...] = midway + arrived(zr2, z2sem)

    part = idv.at[pl.ds(0, ND - 1)]
    remote(part, part, zsem.at[0], zsem.at[1], (d, mate)).wait_send()
    part = rows_s.at[pl.ds(0, ND - 1)]
    remote(part, part, zsem.at[2], zsem.at[3], (d, mate)).wait_send()
    for buf, sem in ((abuf, asem), (ebuf, esem), (fbuf, fsem), (mbuf, msem)):
        gather_sent(buf, sem)

    @pl.loop(0, LOW)
    def _(j):
        @pl.when(j != me)
        def _():
            piece = wts.at[pl.ds(0, 32), :]
            remote(piece, piece, wsem.at[j], wrecv, (d, mate)).wait_send()

    @pl.when(me < LOW)
    def _():
        part = lt.at[pl.ds(0, NM - 1)]
        remote(part, part, ltsend, ltrecv.at[0], (d, mate)).wait_send()

    remote(wo_own, wo_own, psem.at[1], psem.at[2], (d, mate)).wait_send()
    remote(wdn_own, wdn_own, psem.at[4], psem.at[5], (d, mate)).wait_send()
    for buf, sem in ((zs, z1sem), (zs2, z2sem)):
        remote(buf, buf, sem.at[0], sem.at[1], (d, mate)).wait_send()


def write_out(*refs):
    sem = refs[10]
    copies = [pltpu.make_async_copy(refs[i], refs[5 + i], sem.at[i]) for i in (0, 2, 3, 4)]
    for i in range(8):
        part = pl.ds(8 * i, 8)
        copies.append(pltpu.make_async_copy(refs[1].at[part], refs[6].at[part], sem.at[5 + i]))
    for k in copies:
        k.start()
    for k in copies:
        k.wait()


def per_device(
    ids, table, g1, b1, g2, b2, prior_rec, lerp, wd1, wd2, fbase, wa1, wa2, abase, wg1, wg2, erase, lcoef, reward,
    wr, wk, wv, state, clg, clb, wo, g3, b3, prior_ffn, lerp_ffn, wup, wdn,
):
    line = lambda x: x.reshape(1, 128)
    vocab = table.shape[0]
    operands = (
        ids.reshape(1, 64), table.reshape(vocab // 8, 8, 128), prior_rec, lerp, wd1, wd2, wa1, wa2, wg1.T, wg2,
        wr, wk, wv, state, wo, prior_ffn, wup, wdn,
        *map(line, (g1, b1, g2, b2, g3, b3, lerp_ffn, fbase, abase, erase, lcoef, reward, clg, clb)),
    )
    vmem = pltpu.VMEM
    dma = pltpu.SemaphoreType.DMA
    scratch = [
        vmem((ND, 1, 64), jnp.int32), pltpu.SMEM((ND, 1, 64), jnp.int32), vmem((vocab // 8, 8, 128), BF16),
        vmem((14, 1, 128), BF16), vmem((6, 128), BF16),
        vmem((128, 128), BF16), vmem((128, 128), BF16), vmem((128, 128), BF16), vmem((128, 128), BF16),
        vmem((480, 128), BF16),
        vmem((N, 128), BF16), vmem((N, 128), BF16), vmem((N, 128), BF16), vmem((64, 2, 64, 64), F32),
        vmem((256, 2048), BF16), vmem((N, 512), BF16), vmem((1024, 2048), BF16),
        vmem((64, 2, 64, 64), F32), vmem((64, 64, 128), F32),
        vmem((ND, 64, 128), BF16), vmem((ND, 64, 128), BF16),
        vmem((2, NQ, 80, 128), BF16), vmem((2, NQ, 64, 128), BF16), vmem((2, NQ, 64, 128), BF16), vmem((2, NQ, 64, 128), BF16),
        vmem((736, 128), BF16), vmem((32, N), BF16), vmem((4, 64, N), BF16), vmem((2, NQ, 64, 128), F32),
        vmem((2, NQ, 64, 128), BF16), vmem((NM, 16, 128), BF16), vmem((5, 2, 64, 128), F32), vmem((2, 64, 128), F32),
        vmem((2, 64, 128), BF16), vmem((4, 64, 512), F32),
        vmem((NQ, 64, 128), BF16), vmem((NQ, 64, 128), BF16), vmem((NQ, 64, 128), BF16), vmem((NQ, 64, 128), BF16),
        vmem((2, 64, 512), BF16),
        dma((32,)), dma((4,)), dma((3,)), dma((3,)), dma((3,)), dma((3,)), dma((NQ,)), dma((NQ,)), dma((NQ,)), dma((NQ,)), dma((LOW,)), dma, dma, dma((LOW,)),
        dma((7,)), dma((2,)), dma((2,)), dma((4,)),
    ]
    anywhere = pl.BlockSpec(memory_space=pltpu.HBM)
    inside = pl.BlockSpec(memory_space=pltpu.VMEM)
    shapes = (((64, 128), F32), (state.shape, F32), ((64, 128), BF16), ((64, 128), BF16), ((64, 128), BF16))
    kept = pl.pallas_call(
        whole_step,
        name="whole_step",
        out_shape=tuple(pltpu.VMEM(*x) for x in shapes),
        in_specs=[anywhere] * len(operands),
        out_specs=[inside] * 5,
        scratch_shapes=scratch,
        compiler_params=pltpu.CompilerParams(
            collective_id=0, has_side_effects=True, vmem_limit_bytes=VMEM_GRANT
        ),
    )(*operands)
    return pl.pallas_call(
        write_out,
        name="write_out",
        out_shape=tuple(jax.ShapeDtypeStruct(*x) for x in shapes),
        in_specs=[inside] * 5,
        out_specs=[anywhere] * 5,
        scratch_shapes=[dma((13,))],
        compiler_params=pltpu.CompilerParams(vmem_limit_bytes=1 << 20),
    )(*kept)


def solution(mesh):
    col = P(None, "mp")
    row = P("mp", None)
    one = P("mp")
    both = P("dp", "mp")
    return jax.shard_map(
        per_device,
        mesh=mesh,
        in_specs=(
            P("dp"), both, one, one, one, one, both, col, row, col, one, row, col, one, row, col, one, one, one,
            col, col, col, P("dp", "mp", None, None), one, one, row, one, one, both, one, col, row,
        ),
        out_specs=(both, P("dp", "mp", None, None), both, both, both),
        check_vma=False,
    )
```

```python
import jax
import jax.numpy as jnp
from jax import lax
from jax.experimental import pallas as pl
from jax.experimental.pallas import tpu as pltpu
from jax.sharding import PartitionSpec as P

MESH = pl.DeviceIdType.MESH
F32 = jnp.float32
BF16 = jnp.bfloat16
N = 4096
NQ = 16
NM = 32
ND = 4
LOW = 23
V_D, V_RKA, V_W, V_V, V_REM = range(5)
VMEM_GRANT = 62_767_104
FAR = sorted(
    ((dy, dx) for dy in range(4) for dx in range(4) if dy or dx),
    key=lambda o: -min(o[0], 4 - o[0]) - min(o[1], 4 - o[1]),
)
E_HALF = 0.6065306597126334


def whole_step(
    ids, table, prior_rec, lerp, wd1, wd2, wa1, wa2, wg1, wg2, wr, wk, wv, state, wo, prior_ffn, wup, wdn,
    g1, b1, g2, b2, g3, b3, lerp_ffn, fbase, abase, erase, lcoef, reward, clg, clb,
    ov_h, out_s, ov_att, ov_ffn, ov_v,
    idv, ids_s, tab, prm, lerp_v, wd1_v, wd2_v, wa1_v, wa2_v, wg2_v, wr_v, wk_v, wv_v, s_v,
    wop, wup_v, wdp, si, st, rows_s, rows_r, abuf, ebuf, fbuf, mbuf, wts, wt, mx, res, att, lt, vec, rowb, ap, zf, zs, zr, zs2, zr2, hp,
    ld, zsem, asem, esem, fsem, msem, agot, egot, fgot, mgot, wsem, wrecv, ltsend, ltrecv, psem, z1sem, z2sem, hsem,
):
    d = lax.axis_index("dp")
    me = lax.axis_index("mp")
    q = me // 2
    c = me % 2
    mate = me + 1 - 2 * c

    def remote(src, dst, ssem, rsem, dev):
        return pltpu.make_async_remote_copy(
            src_ref=src, dst_ref=dst, send_sem=ssem, recv_sem=rsem, device_id=dev, device_id_type=MESH
        )

    def lanes(i):
        return pl.ds(pl.multiple_of(i * 128, 128), 128)

    def chip(dy, dx):
        return (q // 4 + dy) % 4 * 4 + (q % 4 + dx) % 4

    barrier = pltpu.get_barrier_semaphore()
    for i in range(1, ND):
        for m in (me, mate):
            pl.semaphore_signal(barrier, inc=1, device_id=((d + i) % ND, m), device_id_type=MESH)
    for dy, dx in FAR:
        for e in (0, 1):
            pl.semaphore_signal(barrier, inc=1, device_id=(d, 2 * chip(dy, dx) + e), device_id_type=MESH)
    pl.semaphore_signal(barrier, inc=1, device_id=(d, mate), device_id_type=MESH)

    loads = []

    def load(src, dst):
        k = pltpu.make_async_copy(src, dst, ld.at[len(loads)])
        k.start()
        loads.append(k)
        return k

    l_ids = load(ids, idv.at[d])
    l_prm = [
        load(p, prm.at[i])
        for i, p in enumerate((g1, b1, g2, b2, g3, b3, lerp_ffn, fbase, abase, erase, lcoef, reward, clg, clb))
    ]
    l_prm.append(load(lerp, lerp_v))
    l_prior = load(prior_rec, abuf.at[c, q, pl.ds(16, 64), :])
    l_low = [load(wd1, wd1_v), load(wa1, wa1_v), load(wg1, wts.at[pl.ds(256, 480), :])]
    l_tab = load(table, tab)
    l_low2 = [load(wd2, wd2_v), load(wa2, wa2_v), load(wg2, wg2_v)]
    l_priorf = load(prior_ffn, fbuf.at[c, q])

    for k in l_prm:
        k.wait()
    par = lambda i: prm[i].astype(F32)
    lerp_own = lerp_v[...].astype(F32)
    packed = jnp.concatenate(
        [par(0), par(1), par(2), par(3), lerp_own, par(4), par(5), par(6), jnp.zeros((3, 128), F32)], axis=0
    )
    abuf[c, q, 0:16, :] = packed.astype(BF16)
    for k in l_low:
        k.wait()
    wts[0:128, :] = jnp.transpose(wd1_v[...].astype(F32)).astype(BF16)
    wts[128:256, :] = jnp.transpose(wa1_v[...].astype(F32)).astype(BF16)
    @pl.loop(0, 64)
    def _(i):
        for h in (0, 1):
            pltpu.make_async_copy(state.at[:, h, i, :], si.at[i, h], psem.at[6]).start()

    l_rkv = [load(wk, wk_v), load(wv, wv_v), load(wr, wr_v)]
    l_ids.wait()
    l_prior.wait()

    pl.semaphore_wait(barrier, 2 * (ND - 1) + NM - 1)

    for i in (2, 1, 3):
        remote(idv.at[d], idv.at[d], zsem.at[0], zsem.at[1], ((d + i) % ND, mate)).start()

    def gather_start(buf, sem, got, p):
        for dy, dx in FAR:
            remote(buf.at[p, q], buf.at[p, q], sem.at[0], got.at[q], (d, 2 * chip(dy, dx) + 1 - c)).start()
        remote(buf.at[p, q], buf.at[p, q], sem.at[0], got.at[q], (d, mate)).start()

    def gather_pass_on(buf, sem, got, p, use=None, acc=None):
        for dy, dx in FAR[::-1]:
            t = chip(dy, dx)
            remote(buf.at[1 - p, t], buf.at[1 - p, t], sem.at[0], got.at[t], (d, mate)).wait_recv()
            remote(buf.at[1 - p, t], buf.at[1 - p, t], sem.at[1], sem.at[2], (d, mate)).start()
            if use is not None:
                acc = use(1 - p, t, acc)
        return acc

    def gather_end(buf, sem, got, p):
        remote(buf.at[1 - p, q], buf.at[1 - p, q], sem.at[0], got.at[q], (d, mate)).wait_recv()
        part = buf.at[0, pl.ds(0, NQ - 1)]
        remote(part, part, sem.at[1], sem.at[2], (d, mate)).wait_recv()

    def gather_sent(buf, sem):
        remote(buf.at[0], buf.at[0], sem.at[0], sem.at[2], (d, mate)).wait_send()
        part = buf.at[0, pl.ds(0, NQ - 1)]
        remote(part, part, sem.at[1], sem.at[2], (d, mate)).wait_send()

    gather_start(abuf, asem, agot, c)

    @pl.loop(0, LOW)
    def _(j):
        @pl.when(j != me)
        def _():
            remote(
                wts.at[pl.ds(pl.multiple_of(j * 32, 32), 32), :], wt.at[:, lanes(me)], wsem.at[j], wrecv, (d, j)
            ).start()

    @pl.when(me < LOW)
    def _():
        wt[:, lanes(me)] = wts[pl.ds(pl.multiple_of(me * 32, 32), 32), :]

    own_w = []
    for t in range(NQ):
        own_w.append(
            (
                pltpu.make_async_copy(
                    wo.at[:, lanes(2 * t + 1 - c)],
                    wop.at[pl.ds(pl.multiple_of(c * 128, 128), 128), pl.ds(t * 128, 128)],
                    psem.at[0],
                ),
                remote(
                    wo.at[:, lanes(2 * t + c)],
                    wop.at[pl.ds(pl.multiple_of(c * 128, 128), 128), pl.ds(t * 128, 128)],
                    psem.at[1],
                    psem.at[2],
                    (d, mate),
                ),
                pltpu.make_async_copy(
                    wdn.at[:, lanes(2 * t + 1 - c)],
                    wdp.at[pl.ds(pl.multiple_of(c * 512, 512), 512), pl.ds(t * 128, 128)],
                    psem.at[3],
                ),
                remote(
                    wdn.at[:, lanes(2 * t + c)],
                    wdp.at[pl.ds(pl.multiple_of(c * 512, 512), 512), pl.ds(t * 128, 128)],
                    psem.at[4],
                    psem.at[5],
                    (d, mate),
                ),
            )
        )
    for k in own_w:
        k[0].start()
        k[1].start()
    l_s = load(state, s_v)
    l_up = load(wup, wup_v)
    for k in own_w:
        k[2].start()
        k[3].start()

    part = idv.at[pl.ds(0, ND - 1)]
    remote(part, part, zsem.at[0], zsem.at[1], (d, mate)).wait_recv()
    k = pltpu.make_async_copy(idv, ids_s, ld.at[len(loads)])
    k.start()
    l_tab.wait()
    k.wait()
    bits = (tab.shape[0] * 8).bit_length() - 1
    sub8 = lax.broadcasted_iota(jnp.int32, (8, 128), 0)

    for i in range(ND):
        s = (d + (2, 1, 3, 0)[i]) % ND

        @pl.loop(0, 8, unroll=4)
        def _(g, s=s, i=i):
            block = jnp.zeros((8, 128), F32)
            for u in range(8):
                token = ids_s[s, 0, g * 8 + u]
                eight = tab[lax.shift_right_logical(token, 3) & (tab.shape[0] - 1)].astype(F32)
                want = jnp.where(lax.shift_right_logical(token, bits) == d, token & 7, 8)
                row = jnp.sum(jnp.where(sub8 == want, eight, 0.0), axis=0, keepdims=True)
                block = jnp.where(sub8 == u, row, block)
            rowb[i % 2, pl.ds(pl.multiple_of(g * 8, 8), 8), :] = block

        rows_s[s] = rowb[i % 2].astype(BF16)
        remote(rows_s.at[s], rows_r.at[d], zsem.at[2], zsem.at[3], (s, mate)).start()

    remote(rows_r, rows_r, zsem.at[2], zsem.at[3], (d, mate)).wait_recv()
    found = rows_r[0].astype(F32)
    for s in range(1, ND):
        found = found + rows_r[s].astype(F32)
    ebuf[1 - c, q] = found.astype(BF16)
    gather_start(ebuf, esem, egot, 1 - c)
    gather_pass_on(abuf, asem, agot, c)
    gather_end(abuf, asem, agot, c)
    l_priorf.wait()
    def rowsum(x):
        return jnp.sum(x, axis=-1, keepdims=True)

    zero = jnp.zeros((64, 128), F32)

    def moments_of(buf, p):
        pivot = rowsum(buf[p, q].astype(F32)) / 128

        def add(cc, t, acc):
            x = buf[cc, t].astype(F32) - pivot
            return acc[0] + x, acc[1] + x * x

        return pivot, add

    def mean_and_scale(pivot, acc):
        shift = rowsum(acc[0]) / N
        return pivot + shift, lax.rsqrt(jnp.maximum(rowsum(acc[1]) / N - shift * shift, 0.0) + 1e-05)

    def gathered_norm(buf, sem, got, p):
        pivot, add = moments_of(buf, p)
        acc = gather_pass_on(buf, sem, got, p, add, (zero, zero))
        gather_end(buf, sem, got, p)
        acc = add(1 - p, q, acc)
        acc = lax.fori_loop(0, NQ, lambda t, acc: add(p, t, acc), acc, unroll=4)
        return mean_and_scale(pivot, acc)

    mean1, inv1 = gathered_norm(ebuf, esem, egot, 1 - c)

    def params(cc, t):
        return abuf[cc, t, 0:16, :].astype(F32)

    def over_blocks(body, init):
        def step(t, acc):
            for cc in (0, 1):
                acc = body(cc, t, acc)
            return acc

        return lax.fori_loop(0, NQ, step, init)

    own_p = params(c, q)
    own_res = (ebuf[c, q].astype(F32) - mean1) * inv1 * own_p[0:1] + own_p[1:2]
    pivot2 = rowsum(own_res) / 128

    def first_norm(cc, t, acc):
        p = params(cc, t)
        r = (ebuf[cc, t].astype(F32) - mean1) * inv1 * p[0:1] + p[1:2]
        res[cc, t] = r
        r = r - pivot2
        return acc[0] + r, acc[1] + r * r

    mean2, inv2 = mean_and_scale(pivot2, over_blocks(first_norm, (zero, zero)))

    @pl.when(me < LOW)
    def _():
        got = wt.at[:, pl.ds(0, (NM - 1) * 128)]
        remote(got, got, wsem.at[0], wrecv, (d, mate)).wait_recv()

    def mixing(cc, t):
        p = params(cc, t)
        base = ((res[cc, t] - mean2) * inv2 * p[2:3] + p[3:4]).astype(BF16)
        att[cc, t] = base
        base = base.astype(F32)
        rate = jnp.where(me < 4, p[5:6], jnp.where(me < 8, p[8:9], p[9:10]))
        return (base + (abuf[cc, t, 16:80, :].astype(F32) - base) * rate).astype(BF16)

    low = 0.0
    for t in range(NQ):
        x = jnp.concatenate([mixing(0, t), mixing(1, t)], axis=1)
        low = low + lax.dot_general(
            wt[:, 256 * t : 256 * t + 256], x, (((1,), (1,)), ((), ())), preferred_element_type=F32
        )
    low = jnp.where(me < 4, jnp.tanh(low), jnp.where(me < 8, low, jax.nn.sigmoid(low)))

    @pl.when(me < LOW)
    def _():
        lt[me] = jnp.concatenate([low[0:16], low[16:32]], axis=1).astype(BF16)
        for dy, dx in FAR:
            for e in (0, 1):
                remote(lt.at[me], lt.at[me], ltsend, ltrecv.at[me], (d, 2 * chip(dy, dx) + e)).start()
        remote(lt.at[me], lt.at[me], ltsend, ltrecv.at[me], (d, mate)).start()

    gather_start(fbuf, fsem, fgot, c)

    def mixing_rest(cc, t, acc):
        p = params(cc, t)
        base = att[cc, t].astype(F32)
        delta = abuf[cc, t, 16:80, :].astype(F32) - base
        at = lanes(2 * t + cc)
        mx[1, :, at] = (base + delta * p[6:7]).astype(BF16)
        mx[2, :, at] = (base + delta * p[7:8]).astype(BF16)
        mx[3, :, at] = (base + delta * p[4:5]).astype(BF16)
        return acc

    over_blocks(mixing_rest, 0)
    ov_att[...] = att[c, q]

    def head_rows(i, x):
        vec[i, 0] = x
        vec[i, 1] = pltpu.roll(x, 64, axis=1)

    left = lax.broadcasted_iota(jnp.int32, (64, 128), 1) < 64
    eye = lax.broadcasted_iota(jnp.int32, (64, 64), 0) == lax.broadcasted_iota(jnp.int32, (64, 64), 1)

    def headsum(x):
        return jnp.where(left, rowsum(jnp.where(left, x, 0.0)), rowsum(jnp.where(left, 0.0, x)))

    def projected(i, w, k):
        k.wait()
        return jnp.dot(mx[i], w[...], preferred_element_type=F32)

    def turned(x):
        y = jnp.transpose(x)
        return jnp.concatenate([y[0:64], y[64:128]], axis=1)

    def state_times(x):
        y = turned(x)

        @pl.loop(0, 64, unroll=8)
        def _(i):
            rowb[0, pl.ds(i, 1), :] = jnp.sum(st[i] * y, axis=0, keepdims=True)

        return turned(rowb[0])

    keys = projected(1, wk_v, l_rkv[0])
    removal = keys * par(9)
    removal = removal * lax.rsqrt(headsum(removal * removal) + 1e-06)
    values = projected(2, wv_v, l_rkv[1])
    recept = projected(3, wr_v, l_rkv[2])
    ov_v[...] = values.astype(BF16)
    head_rows(V_V, values)
    pltpu.make_async_copy(si, si, psem.at[6]).wait()

    @pl.loop(0, 64, unroll=4)
    def _(i):
        st[i] = jnp.transpose(si[i].reshape(128, 64))

    removed = state_times(removal)
    head_rows(V_REM, removed)

    for k in l_low2:
        k.wait()

    @pl.loop(0, LOW)
    def _(j):
        @pl.when(j != me)
        def _():
            remote(lt.at[j], lt.at[j], ltsend, ltrecv.at[j], (d, mate)).wait_recv()

    def second(lo, hi, w):
        n = hi - lo
        low = jnp.transpose(lt[lo:hi].astype(F32).reshape(n * 16, 128)).astype(BF16)
        parts = [jnp.concatenate([w[32 * j + 16 * u : 32 * j + 16 * u + 16, :] for j in range(n)], axis=0) for u in (0, 1)]
        return jnp.dot(low[0:64], parts[0], preferred_element_type=F32) + jnp.dot(
            low[64:128], parts[1], preferred_element_type=F32
        )

    decay = jnp.exp(-E_HALF * jax.nn.sigmoid(par(7) + second(0, 4, wd2_v)))
    alpha = jax.nn.sigmoid(par(8) + second(4, 8, wa2_v))
    gate = second(8, LOW, wg2_v)
    written = keys * (1.0 + (alpha - 1.0) * par(10))
    rka = removal * alpha
    head_rows(V_D, decay)
    head_rows(V_RKA, rka)
    head_rows(V_W, written)
    readout = (
        state_times(decay * recept) - removed * headsum(rka * recept) + values * headsum(written * recept)
    )
    centered = readout - headsum(readout) / 64
    normed = centered * lax.rsqrt(headsum(centered * centered) / 64 + 0.00064) * par(12) + par(13)
    bonus = headsum(recept * written * par(11)) * values
    ap[c] = ((normed + bonus) * gate).astype(BF16)
    k = remote(ap.at[c], ap.at[c], hsem.at[0], hsem.at[1], (d, mate))
    k.start()

    wo_own = wop.at[pl.ds(0, 128), :]
    pltpu.make_async_copy(wo_own, wo_own, psem.at[0]).wait()
    remote(wo_own, wo_own, psem.at[1], psem.at[2], (d, mate)).wait_recv()
    def scatter(own, other, w, width, send, recv, sem, copies):
        step = width // len(own)

        def rows_of(p, i):
            return pl.ds(pl.multiple_of(p * width + i * step, step), step)

        rows = [(q // 4 + dy) % 4 for dy in (2, 1, 3, 0)]
        cols = [pl.ds(pl.multiple_of(t * 512, 512), 512) for t in rows]
        terms = [(x, rows_of(c, i)) for i, x in enumerate(own)]
        j = len(own) - 1
        for i in range(j):
            copies[i].wait()
            terms.append((other(i), rows_of(1 - c, i)))
        for i in range(4):
            zf[i] = sum(jnp.dot(x, w[r, cols[i]], preferred_element_type=F32) for x, r in terms)
        copies[j].wait()
        last = other(j)
        for i in range(4):
            y = zf[i] + jnp.dot(last, w[rows_of(1 - c, j), cols[i]], preferred_element_type=F32)
            for u in range(4):
                to = 4 * rows[i] + u
                send[to] = y[:, 128 * u : 128 * u + 128].astype(BF16)
            for dx in (2, 1, 3, 0):
                to = 4 * rows[i] + (q % 4 + dx) % 4
                remote(send.at[to], recv.at[q], sem.at[0], sem.at[1], (d, 2 * to + 1 - c)).start()

    def arrived(recv, sem):
        remote(recv, recv, sem.at[0], sem.at[1], (d, mate)).wait_recv()
        total = recv[0].astype(F32)
        for t in range(1, NQ):
            total = total + recv[t].astype(F32)
        return total

    scatter([ap[c]], lambda i: ap[1 - c], wop, 128, zs, zr, z1sem, [k])

    l_s.wait()

    @pl.loop(0, 64, unroll=4)
    def _(b):
        for h in (0, 1):
            row = lambda i: vec[i, h, pl.ds(b, 1), 0:64]
            gone = rowsum(jnp.where(eye, row(V_REM), 0.0))
            val = rowsum(jnp.where(eye, row(V_V), 0.0))
            out_s[b, h] = s_v[b, h] * row(V_D) - gone * row(V_RKA) + val * row(V_W)


    gather_pass_on(fbuf, fsem, fgot, c)
    midway = own_res + arrived(zr, z1sem)
    mbuf[c, q] = midway.astype(BF16)
    gather_start(mbuf, msem, mgot, c)
    gather_end(fbuf, fsem, fgot, c)
    mean3, inv3 = gathered_norm(mbuf, msem, mgot, c)

    def ffn_mixed(cc, t):
        p = params(cc, t)
        base = ((mbuf[cc, t].astype(F32) - mean3) * inv3 * p[10:11] + p[11:12]).astype(BF16).astype(F32)
        return (base + (fbuf[cc, t].astype(F32) - base) * p[12:13]).astype(BF16)

    l_up.wait()
    up = 0.0
    for t in range(NQ):
        x = jnp.concatenate([ffn_mixed(0, t), ffn_mixed(1, t)], axis=1)
        mx[0, :, 256 * t : 256 * t + 256] = x
        up = up + jnp.dot(x, wup_v[256 * t : 256 * t + 256, 0:256], preferred_element_type=F32)
    hp[0, c] = jnp.square(jnp.maximum(up, 0.0)).astype(BF16)
    halves = [remote(hp.at[i, c], hp.at[i, c], hsem.at[2 + 2 * i], hsem.at[3 + 2 * i], (d, mate)) for i in (0, 1)]
    halves[0].start()
    up = jnp.dot(mx[0], wup_v[:, 256:512], preferred_element_type=F32)
    hp[1, c] = jnp.square(jnp.maximum(up, 0.0)).astype(BF16)
    halves[1].start()
    ov_ffn[...] = ((midway - mean3) * inv3 * par(4) + par(5)).astype(BF16)
    wdn_own = wdp.at[pl.ds(0, 512), :]
    pltpu.make_async_copy(wdn_own, wdn_own, psem.at[3]).wait()
    remote(wdn_own, wdn_own, psem.at[4], psem.at[5], (d, mate)).wait_recv()
    scatter([hp[0, c], hp[1, c]], lambda i: hp[i, 1 - c], wdp, 512, zs2, zr2, z2sem, halves)
    ov_h[...] = midway + arrived(zr2, z2sem)

    part = idv.at[pl.ds(0, ND - 1)]
    remote(part, part, zsem.at[0], zsem.at[1], (d, mate)).wait_send()
    remote(rows_s, rows_s, zsem.at[2], zsem.at[3], (d, mate)).wait_send()
    for buf, sem in ((abuf, asem), (ebuf, esem), (fbuf, fsem), (mbuf, msem)):
        gather_sent(buf, sem)

    @pl.loop(0, LOW)
    def _(j):
        @pl.when(j != me)
        def _():
            piece = wts.at[pl.ds(0, 32), :]
            remote(piece, piece, wsem.at[j], wrecv, (d, mate)).wait_send()

    @pl.when(me < LOW)
    def _():
        part = lt.at[pl.ds(0, NM - 1)]
        remote(part, part, ltsend, ltrecv.at[0], (d, mate)).wait_send()

    remote(wo_own, wo_own, psem.at[1], psem.at[2], (d, mate)).wait_send()
    remote(wdn_own, wdn_own, psem.at[4], psem.at[5], (d, mate)).wait_send()
    for buf, sem in ((zs, z1sem), (zs2, z2sem)):
        remote(buf, buf, sem.at[0], sem.at[1], (d, mate)).wait_send()


def write_out(*refs):
    sem = refs[10]
    copies = [pltpu.make_async_copy(refs[i], refs[5 + i], sem.at[i]) for i in (0, 2, 3, 4)]
    for i in range(8):
        part = pl.ds(8 * i, 8)
        copies.append(pltpu.make_async_copy(refs[1].at[part], refs[6].at[part], sem.at[5 + i]))
    for k in copies:
        k.start()
    for k in copies:
        k.wait()


def per_device(
    ids, table, g1, b1, g2, b2, prior_rec, lerp, wd1, wd2, fbase, wa1, wa2, abase, wg1, wg2, erase, lcoef, reward,
    wr, wk, wv, state, clg, clb, wo, g3, b3, prior_ffn, lerp_ffn, wup, wdn,
):
    line = lambda x: x.reshape(1, 128)
    vocab = table.shape[0]
    operands = (
        ids.reshape(1, 64), table.reshape(vocab // 8, 8, 128), prior_rec, lerp, wd1, wd2, wa1, wa2, wg1.T, wg2,
        wr, wk, wv, state, wo, prior_ffn, wup, wdn,
        *map(line, (g1, b1, g2, b2, g3, b3, lerp_ffn, fbase, abase, erase, lcoef, reward, clg, clb)),
    )
    vmem = pltpu.VMEM
    dma = pltpu.SemaphoreType.DMA
    scratch = [
        vmem((ND, 1, 64), jnp.int32), pltpu.SMEM((ND, 1, 64), jnp.int32), vmem((vocab // 8, 8, 128), BF16),
        vmem((14, 1, 128), BF16), vmem((6, 128), BF16),
        vmem((128, 128), BF16), vmem((128, 128), BF16), vmem((128, 128), BF16), vmem((128, 128), BF16),
        vmem((480, 128), BF16),
        vmem((N, 128), BF16), vmem((N, 128), BF16), vmem((N, 128), BF16), vmem((64, 2, 64, 64), F32),
        vmem((256, 2048), BF16), vmem((N, 512), BF16), vmem((1024, 2048), BF16),
        vmem((64, 2, 64, 64), F32), vmem((64, 64, 128), F32),
        vmem((ND, 64, 128), BF16), vmem((ND, 64, 128), BF16),
        vmem((2, NQ, 80, 128), BF16), vmem((2, NQ, 64, 128), BF16), vmem((2, NQ, 64, 128), BF16), vmem((2, NQ, 64, 128), BF16),
        vmem((736, 128), BF16), vmem((32, N), BF16), vmem((4, 64, N), BF16), vmem((2, NQ, 64, 128), F32),
        vmem((2, NQ, 64, 128), BF16), vmem((NM, 16, 128), BF16), vmem((5, 2, 64, 128), F32), vmem((2, 64, 128), F32),
        vmem((2, 64, 128), BF16), vmem((4, 64, 512), F32),
        vmem((NQ, 64, 128), BF16), vmem((NQ, 64, 128), BF16), vmem((NQ, 64, 128), BF16), vmem((NQ, 64, 128), BF16),
        vmem((2, 2, 64, 256), BF16),
        dma((32,)), dma((4,)), dma((3,)), dma((3,)), dma((3,)), dma((3,)), dma((NQ,)), dma((NQ,)), dma((NQ,)), dma((NQ,)), dma((LOW,)), dma, dma, dma((LOW,)),
        dma((7,)), dma((2,)), dma((2,)), dma((6,)),
    ]
    anywhere = pl.BlockSpec(memory_space=pltpu.HBM)
    inside = pl.BlockSpec(memory_space=pltpu.VMEM)
    shapes = (((64, 128), F32), (state.shape, F32), ((64, 128), BF16), ((64, 128), BF16), ((64, 128), BF16))
    kept = pl.pallas_call(
        whole_step,
        name="whole_step",
        out_shape=tuple(pltpu.VMEM(*x) for x in shapes),
        in_specs=[anywhere] * len(operands),
        out_specs=[inside] * 5,
        scratch_shapes=scratch,
        compiler_params=pltpu.CompilerParams(
            collective_id=0, has_side_effects=True, vmem_limit_bytes=VMEM_GRANT
        ),
    )(*operands)
    return pl.pallas_call(
        write_out,
        name="write_out",
        out_shape=tuple(jax.ShapeDtypeStruct(*x) for x in shapes),
        in_specs=[inside] * 5,
        out_specs=[anywhere] * 5,
        scratch_shapes=[dma((13,))],
        compiler_params=pltpu.CompilerParams(vmem_limit_bytes=1 << 20),
    )(*kept)


def solution(mesh):
    col = P(None, "mp")
    row = P("mp", None)
    one = P("mp")
    both = P("dp", "mp")
    return jax.shard_map(
        per_device,
        mesh=mesh,
        in_specs=(
            P("dp"), both, one, one, one, one, both, col, row, col, one, row, col, one, row, col, one, one, one,
            col, col, col, P("dp", "mp", None, None), one, one, row, one, one, both, one, col, row,
        ),
        out_specs=(both, P("dp", "mp", None, None), both, both, both),
        check_vma=False,
    )
```

```python
import jax
import jax.numpy as jnp
from jax import lax
from jax.experimental import pallas as pl
from jax.experimental.pallas import tpu as pltpu
from jax.sharding import PartitionSpec as P

MESH = pl.DeviceIdType.MESH
F32 = jnp.float32
BF16 = jnp.bfloat16
N = 4096
NQ = 16
NM = 32
ND = 4
LOW = 23
V_D, V_RKA, V_W, V_V, V_REM = range(5)
VMEM_GRANT = 62_767_104
FAR = sorted(
    ((dy, dx) for dy in range(4) for dx in range(4) if dy or dx),
    key=lambda o: -min(o[0], 4 - o[0]) - min(o[1], 4 - o[1]),
)
E_HALF = 0.6065306597126334


def whole_step(
    ids, table, prior_rec, lerp, wd1, wd2, wa1, wa2, wg1, wg2, wr, wk, wv, state, wo, prior_ffn, wup, wdn,
    g1, b1, g2, b2, g3, b3, lerp_ffn, fbase, abase, erase, lcoef, reward, clg, clb,
    ov_h, out_s, ov_att, ov_ffn, ov_v,
    idv, ids_s, tab, prm, lerp_v, wd1_v, wd2_v, wa1_v, wa2_v, wg2_v, wr_v, wk_v, wv_v, s_v,
    wop, wup_v, wdp, si, st, rows_s, rows_r, abuf, ebuf, fbuf, mbuf, wts, wt, mx, res, att, lt, vec, rowb, ap, zf, zs, zr, zs2, zr2, hp,
    ld, zsem, asem, esem, fsem, msem, agot, egot, fgot, mgot, wsem, wrecv, ltsend, ltrecv, psem, z1sem, z2sem, hsem,
):
    d = lax.axis_index("dp")
    me = lax.axis_index("mp")
    q = me // 2
    c = me % 2
    mate = me + 1 - 2 * c

    def remote(src, dst, ssem, rsem, dev):
        return pltpu.make_async_remote_copy(
            src_ref=src, dst_ref=dst, send_sem=ssem, recv_sem=rsem, device_id=dev, device_id_type=MESH
        )

    def lanes(i):
        return pl.ds(pl.multiple_of(i * 128, 128), 128)

    def chip(dy, dx):
        return (q // 4 + dy) % 4 * 4 + (q % 4 + dx) % 4

    barrier = pltpu.get_barrier_semaphore()
    for i in range(1, ND):
        for m in (me, mate):
            pl.semaphore_signal(barrier, inc=1, device_id=((d + i) % ND, m), device_id_type=MESH)
    for dy, dx in FAR:
        for e in (0, 1):
            pl.semaphore_signal(barrier, inc=1, device_id=(d, 2 * chip(dy, dx) + e), device_id_type=MESH)
    pl.semaphore_signal(barrier, inc=1, device_id=(d, mate), device_id_type=MESH)

    loads = []

    def load(src, dst):
        k = pltpu.make_async_copy(src, dst, ld.at[len(loads)])
        k.start()
        loads.append(k)
        return k

    l_ids = load(ids, idv.at[d])
    l_prm = [
        load(p, prm.at[i])
        for i, p in enumerate((g1, b1, g2, b2, g3, b3, lerp_ffn, fbase, abase, erase, lcoef, reward, clg, clb))
    ]
    l_prm.append(load(lerp, lerp_v))
    l_prior = load(prior_rec, abuf.at[c, q, pl.ds(16, 64), :])
    l_low = [load(wd1, wd1_v), load(wa1, wa1_v), load(wg1, wts.at[pl.ds(256, 480), :])]
    l_tab = load(table, tab)
    l_low2 = [load(wd2, wd2_v), load(wa2, wa2_v), load(wg2, wg2_v)]
    l_priorf = load(prior_ffn, fbuf.at[c, q])

    for k in l_prm:
        k.wait()
    par = lambda i: prm[i].astype(F32)
    lerp_own = lerp_v[...].astype(F32)
    packed = jnp.concatenate(
        [par(0), par(1), par(2), par(3), lerp_own, par(4), par(5), par(6), jnp.zeros((3, 128), F32)], axis=0
    )
    abuf[c, q, 0:16, :] = packed.astype(BF16)
    for k in l_low:
        k.wait()
    wts[0:128, :] = jnp.transpose(wd1_v[...].astype(F32)).astype(BF16)
    wts[128:256, :] = jnp.transpose(wa1_v[...].astype(F32)).astype(BF16)
    @pl.loop(0, 64)
    def _(i):
        for h in (0, 1):
            pltpu.make_async_copy(state.at[:, h, i, :], si.at[i, h], psem.at[6]).start()

    l_rkv = [load(wk, wk_v), load(wv, wv_v), load(wr, wr_v)]
    l_ids.wait()
    l_prior.wait()

    pl.semaphore_wait(barrier, 2 * (ND - 1) + NM - 1)

    for i in (2, 1, 3):
        remote(idv.at[d], idv.at[d], zsem.at[0], zsem.at[1], ((d + i) % ND, mate)).start()

    def gather_start(buf, sem, got, p):
        for dy, dx in FAR:
            remote(buf.at[p, q], buf.at[p, q], sem.at[0], got.at[q], (d, 2 * chip(dy, dx) + 1 - c)).start()
        remote(buf.at[p, q], buf.at[p, q], sem.at[0], got.at[q], (d, mate)).start()

    def gather_pass_on(buf, sem, got, p, use=None, acc=None):
        for dy, dx in FAR[::-1]:
            t = chip(dy, dx)
            remote(buf.at[1 - p, t], buf.at[1 - p, t], sem.at[0], got.at[t], (d, mate)).wait_recv()
            remote(buf.at[1 - p, t], buf.at[1 - p, t], sem.at[1], sem.at[2], (d, mate)).start()
            if use is not None:
                acc = use(1 - p, t, acc)
        return acc

    def gather_end(buf, sem, got, p):
        remote(buf.at[1 - p, q], buf.at[1 - p, q], sem.at[0], got.at[q], (d, mate)).wait_recv()
        part = buf.at[0, pl.ds(0, NQ - 1)]
        remote(part, part, sem.at[1], sem.at[2], (d, mate)).wait_recv()

    def gather_sent(buf, sem):
        remote(buf.at[0], buf.at[0], sem.at[0], sem.at[2], (d, mate)).wait_send()
        part = buf.at[0, pl.ds(0, NQ - 1)]
        remote(part, part, sem.at[1], sem.at[2], (d, mate)).wait_send()

    gather_start(abuf, asem, agot, c)

    @pl.loop(0, LOW)
    def _(j):
        @pl.when(j != me)
        def _():
            remote(
                wts.at[pl.ds(pl.multiple_of(j * 32, 32), 32), :], wt.at[:, lanes(me)], wsem.at[j], wrecv, (d, j)
            ).start()

    @pl.when(me < LOW)
    def _():
        wt[:, lanes(me)] = wts[pl.ds(pl.multiple_of(me * 32, 32), 32), :]

    own_w = []
    for t in range(NQ):
        own_w.append(
            (
                pltpu.make_async_copy(
                    wo.at[:, lanes(2 * t + 1 - c)],
                    wop.at[pl.ds(pl.multiple_of(c * 128, 128), 128), pl.ds(t * 128, 128)],
                    psem.at[0],
                ),
                remote(
                    wo.at[:, lanes(2 * t + c)],
                    wop.at[pl.ds(pl.multiple_of(c * 128, 128), 128), pl.ds(t * 128, 128)],
                    psem.at[1],
                    psem.at[2],
                    (d, mate),
                ),
                pltpu.make_async_copy(
                    wdn.at[:, lanes(2 * t + 1 - c)],
                    wdp.at[pl.ds(pl.multiple_of(c * 512, 512), 512), pl.ds(t * 128, 128)],
                    psem.at[3],
                ),
                remote(
                    wdn.at[:, lanes(2 * t + c)],
                    wdp.at[pl.ds(pl.multiple_of(c * 512, 512), 512), pl.ds(t * 128, 128)],
                    psem.at[4],
                    psem.at[5],
                    (d, mate),
                ),
            )
        )
    for k in own_w:
        k[0].start()
        k[1].start()
    l_s = load(state, s_v)
    l_up = load(wup, wup_v)
    for k in own_w:
        k[2].start()
        k[3].start()

    part = idv.at[pl.ds(0, ND - 1)]
    remote(part, part, zsem.at[0], zsem.at[1], (d, mate)).wait_recv()
    k = pltpu.make_async_copy(idv, ids_s, ld.at[len(loads)])
    k.start()
    l_tab.wait()
    k.wait()
    bits = (tab.shape[0] * 8).bit_length() - 1
    sub8 = lax.broadcasted_iota(jnp.int32, (8, 128), 0)

    for i in range(ND):
        s = (d + (2, 1, 3, 0)[i]) % ND

        @pl.loop(0, 8, unroll=8)
        def _(g, s=s, i=i):
            block = jnp.zeros((8, 128), F32)
            for u in range(8):
                token = ids_s[s, 0, g * 8 + u]
                eight = tab[lax.shift_right_logical(token, 3) & (tab.shape[0] - 1)].astype(F32)
                want = jnp.where(lax.shift_right_logical(token, bits) == d, token & 7, 8)
                row = jnp.sum(jnp.where(sub8 == want, eight, 0.0), axis=0, keepdims=True)
                block = jnp.where(sub8 == u, row, block)
            rowb[i % 2, pl.ds(pl.multiple_of(g * 8, 8), 8), :] = block

        rows_s[s] = rowb[i % 2].astype(BF16)
        remote(rows_s.at[s], rows_r.at[d], zsem.at[2], zsem.at[3], (s, mate)).start()

    remote(rows_r, rows_r, zsem.at[2], zsem.at[3], (d, mate)).wait_recv()
    found = rows_r[0].astype(F32)
    for s in range(1, ND):
        found = found + rows_r[s].astype(F32)
    ebuf[1 - c, q] = found.astype(BF16)
    gather_start(ebuf, esem, egot, 1 - c)
    gather_pass_on(abuf, asem, agot, c)
    gather_end(abuf, asem, agot, c)
    l_priorf.wait()
    def rowsum(x):
        return jnp.sum(x, axis=-1, keepdims=True)

    zero = jnp.zeros((64, 128), F32)

    def moments_of(buf, p):
        pivot = rowsum(buf[p, q].astype(F32)) / 128

        def add(cc, t, acc):
            x = buf[cc, t].astype(F32) - pivot
            return acc[0] + x, acc[1] + x * x

        return pivot, add

    def mean_and_scale(pivot, acc):
        shift = rowsum(acc[0]) / N
        return pivot + shift, lax.rsqrt(jnp.maximum(rowsum(acc[1]) / N - shift * shift, 0.0) + 1e-05)

    def gathered_norm(buf, sem, got, p):
        pivot, add = moments_of(buf, p)
        acc = gather_pass_on(buf, sem, got, p, add, (zero, zero))
        gather_end(buf, sem, got, p)
        acc = add(1 - p, q, acc)
        acc = lax.fori_loop(0, NQ, lambda t, acc: add(p, t, acc), acc, unroll=8)
        return mean_and_scale(pivot, acc)

    mean1, inv1 = gathered_norm(ebuf, esem, egot, 1 - c)

    def params(cc, t):
        return abuf[cc, t, 0:16, :].astype(F32)

    def over_blocks(body, init):
        def step(t, acc):
            for cc in (0, 1):
                acc = body(cc, t, acc)
            return acc

        return lax.fori_loop(0, NQ, step, init, unroll=4)

    own_p = params(c, q)
    own_res = (ebuf[c, q].astype(F32) - mean1) * inv1 * own_p[0:1] + own_p[1:2]
    pivot2 = rowsum(own_res) / 128

    def first_norm(cc, t, acc):
        p = params(cc, t)
        r = (ebuf[cc, t].astype(F32) - mean1) * inv1 * p[0:1] + p[1:2]
        res[cc, t] = r
        r = r - pivot2
        return acc[0] + r, acc[1] + r * r

    mean2, inv2 = mean_and_scale(pivot2, over_blocks(first_norm, (zero, zero)))

    @pl.when(me < LOW)
    def _():
        got = wt.at[:, pl.ds(0, (NM - 1) * 128)]
        remote(got, got, wsem.at[0], wrecv, (d, mate)).wait_recv()

    def mixing(cc, t):
        p = params(cc, t)
        base = ((res[cc, t] - mean2) * inv2 * p[2:3] + p[3:4]).astype(BF16)
        att[cc, t] = base
        base = base.astype(F32)
        rate = jnp.where(me < 4, p[5:6], jnp.where(me < 8, p[8:9], p[9:10]))
        return (base + (abuf[cc, t, 16:80, :].astype(F32) - base) * rate).astype(BF16)

    low = 0.0
    for t in range(NQ):
        x = jnp.concatenate([mixing(0, t), mixing(1, t)], axis=1)
        low = low + lax.dot_general(
            wt[:, 256 * t : 256 * t + 256], x, (((1,), (1,)), ((), ())), preferred_element_type=F32
        )
    low = jnp.where(me < 4, jnp.tanh(low), jnp.where(me < 8, low, jax.nn.sigmoid(low)))

    @pl.when(me < LOW)
    def _():
        lt[me] = jnp.concatenate([low[0:16], low[16:32]], axis=1).astype(BF16)
        for dy, dx in FAR:
            for e in (0, 1):
                remote(lt.at[me], lt.at[me], ltsend, ltrecv.at[me], (d, 2 * chip(dy, dx) + e)).start()
        remote(lt.at[me], lt.at[me], ltsend, ltrecv.at[me], (d, mate)).start()

    gather_start(fbuf, fsem, fgot, c)

    def mixing_rest(cc, t, acc):
        p = params(cc, t)
        base = att[cc, t].astype(F32)
        delta = abuf[cc, t, 16:80, :].astype(F32) - base
        at = lanes(2 * t + cc)
        mx[1, :, at] = (base + delta * p[6:7]).astype(BF16)
        mx[2, :, at] = (base + delta * p[7:8]).astype(BF16)
        mx[3, :, at] = (base + delta * p[4:5]).astype(BF16)
        return acc

    over_blocks(mixing_rest, 0)
    ov_att[...] = att[c, q]

    def head_rows(i, x):
        vec[i, 0] = x
        vec[i, 1] = pltpu.roll(x, 64, axis=1)

    left = lax.broadcasted_iota(jnp.int32, (64, 128), 1) < 64
    eye = lax.broadcasted_iota(jnp.int32, (64, 64), 0) == lax.broadcasted_iota(jnp.int32, (64, 64), 1)

    def headsum(x):
        return jnp.where(left, rowsum(jnp.where(left, x, 0.0)), rowsum(jnp.where(left, 0.0, x)))

    def projected(i, w, k):
        k.wait()
        return jnp.dot(mx[i], w[...], preferred_element_type=F32)

    def turned(x):
        y = jnp.transpose(x)
        return jnp.concatenate([y[0:64], y[64:128]], axis=1)

    def state_times(x):
        y = turned(x)

        @pl.loop(0, 64, unroll=8)
        def _(i):
            rowb[0, pl.ds(i, 1), :] = jnp.sum(st[i] * y, axis=0, keepdims=True)

        return turned(rowb[0])

    keys = projected(1, wk_v, l_rkv[0])
    removal = keys * par(9)
    removal = removal * lax.rsqrt(headsum(removal * removal) + 1e-06)
    values = projected(2, wv_v, l_rkv[1])
    recept = projected(3, wr_v, l_rkv[2])
    ov_v[...] = values.astype(BF16)
    head_rows(V_V, values)
    pltpu.make_async_copy(si, si, psem.at[6]).wait()

    @pl.loop(0, 64, unroll=4)
    def _(i):
        st[i] = jnp.transpose(si[i].reshape(128, 64))

    removed = state_times(removal)
    head_rows(V_REM, removed)

    for k in l_low2:
        k.wait()

    @pl.loop(0, LOW)
    def _(j):
        @pl.when(j != me)
        def _():
            remote(lt.at[j], lt.at[j], ltsend, ltrecv.at[j], (d, mate)).wait_recv()

    def second(lo, hi, w):
        n = hi - lo
        low = jnp.transpose(lt[lo:hi].astype(F32).reshape(n * 16, 128)).astype(BF16)
        parts = [jnp.concatenate([w[32 * j + 16 * u : 32 * j + 16 * u + 16, :] for j in range(n)], axis=0) for u in (0, 1)]
        return jnp.dot(low[0:64], parts[0], preferred_element_type=F32) + jnp.dot(
            low[64:128], parts[1], preferred_element_type=F32
        )

    decay = jnp.exp(-E_HALF * jax.nn.sigmoid(par(7) + second(0, 4, wd2_v)))
    alpha = jax.nn.sigmoid(par(8) + second(4, 8, wa2_v))
    gate = second(8, LOW, wg2_v)
    written = keys * (1.0 + (alpha - 1.0) * par(10))
    rka = removal * alpha
    head_rows(V_D, decay)
    head_rows(V_RKA, rka)
    head_rows(V_W, written)
    readout = (
        state_times(decay * recept) - removed * headsum(rka * recept) + values * headsum(written * recept)
    )
    centered = readout - headsum(readout) / 64
    normed = centered * lax.rsqrt(headsum(centered * centered) / 64 + 0.00064) * par(12) + par(13)
    bonus = headsum(recept * written * par(11)) * values
    ap[c] = ((normed + bonus) * gate).astype(BF16)
    k = remote(ap.at[c], ap.at[c], hsem.at[0], hsem.at[1], (d, mate))
    k.start()

    wo_own = wop.at[pl.ds(0, 128), :]
    pltpu.make_async_copy(wo_own, wo_own, psem.at[0]).wait()
    remote(wo_own, wo_own, psem.at[1], psem.at[2], (d, mate)).wait_recv()
    def scatter(own, other, w, width, send, recv, sem, copies):
        step = width // len(own)

        def rows_of(p, i):
            return pl.ds(pl.multiple_of(p * width + i * step, step), step)

        rows = [(q // 4 + dy) % 4 for dy in (2, 1, 3, 0)]
        cols = [pl.ds(pl.multiple_of(t * 512, 512), 512) for t in rows]
        terms = [(x, rows_of(c, i)) for i, x in enumerate(own)]
        j = len(own) - 1
        for i in range(j):
            copies[i].wait()
            terms.append((other(i), rows_of(1 - c, i)))
        for i in range(4):
            zf[i] = sum(jnp.dot(x, w[r, cols[i]], preferred_element_type=F32) for x, r in terms)
        copies[j].wait()
        last = other(j)
        for i in range(4):
            y = zf[i] + jnp.dot(last, w[rows_of(1 - c, j), cols[i]], preferred_element_type=F32)
            for u in range(4):
                to = 4 * rows[i] + u
                send[to] = y[:, 128 * u : 128 * u + 128].astype(BF16)
            for dx in (2, 1, 3, 0):
                to = 4 * rows[i] + (q % 4 + dx) % 4
                remote(send.at[to], recv.at[q], sem.at[0], sem.at[1], (d, 2 * to + 1 - c)).start()

    def arrived(recv, sem):
        remote(recv, recv, sem.at[0], sem.at[1], (d, mate)).wait_recv()
        total = recv[0].astype(F32)
        for t in range(1, NQ):
            total = total + recv[t].astype(F32)
        return total

    scatter([ap[c]], lambda i: ap[1 - c], wop, 128, zs, zr, z1sem, [k])

    l_s.wait()

    @pl.loop(0, 64, unroll=4)
    def _(b):
        for h in (0, 1):
            row = lambda i: vec[i, h, pl.ds(b, 1), 0:64]
            gone = rowsum(jnp.where(eye, row(V_REM), 0.0))
            val = rowsum(jnp.where(eye, row(V_V), 0.0))
            out_s[b, h] = s_v[b, h] * row(V_D) - gone * row(V_RKA) + val * row(V_W)


    gather_pass_on(fbuf, fsem, fgot, c)
    midway = own_res + arrived(zr, z1sem)
    mbuf[c, q] = midway.astype(BF16)
    gather_start(mbuf, msem, mgot, c)
    gather_end(fbuf, fsem, fgot, c)
    mean3, inv3 = gathered_norm(mbuf, msem, mgot, c)

    def ffn_mixed(cc, t):
        p = params(cc, t)
        base = ((mbuf[cc, t].astype(F32) - mean3) * inv3 * p[10:11] + p[11:12]).astype(BF16).astype(F32)
        return (base + (fbuf[cc, t].astype(F32) - base) * p[12:13]).astype(BF16)

    l_up.wait()
    up = 0.0
    for t in range(NQ):
        x = jnp.concatenate([ffn_mixed(0, t), ffn_mixed(1, t)], axis=1)
        mx[0, :, 256 * t : 256 * t + 256] = x
        up = up + jnp.dot(x, wup_v[256 * t : 256 * t + 256, 0:256], preferred_element_type=F32)
    hp[0, c] = jnp.square(jnp.maximum(up, 0.0)).astype(BF16)
    halves = [remote(hp.at[i, c], hp.at[i, c], hsem.at[2 + 2 * i], hsem.at[3 + 2 * i], (d, mate)) for i in (0, 1)]
    halves[0].start()
    up = jnp.dot(mx[0], wup_v[:, 256:512], preferred_element_type=F32)
    hp[1, c] = jnp.square(jnp.maximum(up, 0.0)).astype(BF16)
    halves[1].start()
    ov_ffn[...] = ((midway - mean3) * inv3 * par(4) + par(5)).astype(BF16)
    wdn_own = wdp.at[pl.ds(0, 512), :]
    pltpu.make_async_copy(wdn_own, wdn_own, psem.at[3]).wait()
    remote(wdn_own, wdn_own, psem.at[4], psem.at[5], (d, mate)).wait_recv()
    scatter([hp[0, c], hp[1, c]], lambda i: hp[i, 1 - c], wdp, 512, zs2, zr2, z2sem, halves)
    ov_h[...] = midway + arrived(zr2, z2sem)

    part = idv.at[pl.ds(0, ND - 1)]
    remote(part, part, zsem.at[0], zsem.at[1], (d, mate)).wait_send()
    remote(rows_s, rows_s, zsem.at[2], zsem.at[3], (d, mate)).wait_send()
    for buf, sem in ((abuf, asem), (ebuf, esem), (fbuf, fsem), (mbuf, msem)):
        gather_sent(buf, sem)

    @pl.loop(0, LOW)
    def _(j):
        @pl.when(j != me)
        def _():
            piece = wts.at[pl.ds(0, 32), :]
            remote(piece, piece, wsem.at[j], wrecv, (d, mate)).wait_send()

    @pl.when(me < LOW)
    def _():
        part = lt.at[pl.ds(0, NM - 1)]
        remote(part, part, ltsend, ltrecv.at[0], (d, mate)).wait_send()

    remote(wo_own, wo_own, psem.at[1], psem.at[2], (d, mate)).wait_send()
    remote(wdn_own, wdn_own, psem.at[4], psem.at[5], (d, mate)).wait_send()
    for buf, sem in ((zs, z1sem), (zs2, z2sem)):
        remote(buf, buf, sem.at[0], sem.at[1], (d, mate)).wait_send()


def write_out(*refs):
    sem = refs[10]
    copies = [pltpu.make_async_copy(refs[i], refs[5 + i], sem.at[i]) for i in (0, 2, 3, 4)]
    for i in range(8):
        part = pl.ds(8 * i, 8)
        copies.append(pltpu.make_async_copy(refs[1].at[part], refs[6].at[part], sem.at[5 + i]))
    for k in copies:
        k.start()
    for k in copies:
        k.wait()


def per_device(
    ids, table, g1, b1, g2, b2, prior_rec, lerp, wd1, wd2, fbase, wa1, wa2, abase, wg1, wg2, erase, lcoef, reward,
    wr, wk, wv, state, clg, clb, wo, g3, b3, prior_ffn, lerp_ffn, wup, wdn,
):
    line = lambda x: x.reshape(1, 128)
    vocab = table.shape[0]
    operands = (
        ids.reshape(1, 64), table.reshape(vocab // 8, 8, 128), prior_rec, lerp, wd1, wd2, wa1, wa2, wg1.T, wg2,
        wr, wk, wv, state, wo, prior_ffn, wup, wdn,
        *map(line, (g1, b1, g2, b2, g3, b3, lerp_ffn, fbase, abase, erase, lcoef, reward, clg, clb)),
    )
    vmem = pltpu.VMEM
    dma = pltpu.SemaphoreType.DMA
    scratch = [
        vmem((ND, 1, 64), jnp.int32), pltpu.SMEM((ND, 1, 64), jnp.int32), vmem((vocab // 8, 8, 128), BF16),
        vmem((14, 1, 128), BF16), vmem((6, 128), BF16),
        vmem((128, 128), BF16), vmem((128, 128), BF16), vmem((128, 128), BF16), vmem((128, 128), BF16),
        vmem((480, 128), BF16),
        vmem((N, 128), BF16), vmem((N, 128), BF16), vmem((N, 128), BF16), vmem((64, 2, 64, 64), F32),
        vmem((256, 2048), BF16), vmem((N, 512), BF16), vmem((1024, 2048), BF16),
        vmem((64, 2, 64, 64), F32), vmem((64, 64, 128), F32),
        vmem((ND, 64, 128), BF16), vmem((ND, 64, 128), BF16),
        vmem((2, NQ, 80, 128), BF16), vmem((2, NQ, 64, 128), BF16), vmem((2, NQ, 64, 128), BF16), vmem((2, NQ, 64, 128), BF16),
        vmem((736, 128), BF16), vmem((32, N), BF16), vmem((4, 64, N), BF16), vmem((2, NQ, 64, 128), F32),
        vmem((2, NQ, 64, 128), BF16), vmem((NM, 16, 128), BF16), vmem((5, 2, 64, 128), F32), vmem((2, 64, 128), F32),
        vmem((2, 64, 128), BF16), vmem((4, 64, 512), F32),
        vmem((NQ, 64, 128), BF16), vmem((NQ, 64, 128), BF16), vmem((NQ, 64, 128), BF16), vmem((NQ, 64, 128), BF16),
        vmem((2, 2, 64, 256), BF16),
        dma((32,)), dma((4,)), dma((3,)), dma((3,)), dma((3,)), dma((3,)), dma((NQ,)), dma((NQ,)), dma((NQ,)), dma((NQ,)), dma((LOW,)), dma, dma, dma((LOW,)),
        dma((7,)), dma((2,)), dma((2,)), dma((6,)),
    ]
    anywhere = pl.BlockSpec(memory_space=pltpu.HBM)
    inside = pl.BlockSpec(memory_space=pltpu.VMEM)
    shapes = (((64, 128), F32), (state.shape, F32), ((64, 128), BF16), ((64, 128), BF16), ((64, 128), BF16))
    kept = pl.pallas_call(
        whole_step,
        name="whole_step",
        out_shape=tuple(pltpu.VMEM(*x) for x in shapes),
        in_specs=[anywhere] * len(operands),
        out_specs=[inside] * 5,
        scratch_shapes=scratch,
        compiler_params=pltpu.CompilerParams(
            collective_id=0, has_side_effects=True, vmem_limit_bytes=VMEM_GRANT
        ),
    )(*operands)
    return pl.pallas_call(
        write_out,
        name="write_out",
        out_shape=tuple(jax.ShapeDtypeStruct(*x) for x in shapes),
        in_specs=[inside] * 5,
        out_specs=[anywhere] * 5,
        scratch_shapes=[dma((13,))],
        compiler_params=pltpu.CompilerParams(vmem_limit_bytes=1 << 20),
    )(*kept)


def solution(mesh):
    col = P(None, "mp")
    row = P("mp", None)
    one = P("mp")
    both = P("dp", "mp")
    return jax.shard_map(
        per_device,
        mesh=mesh,
        in_specs=(
            P("dp"), both, one, one, one, one, both, col, row, col, one, row, col, one, row, col, one, one, one,
            col, col, col, P("dp", "mp", None, None), one, one, row, one, one, both, one, col, row,
        ),
        out_specs=(both, P("dp", "mp", None, None), both, both, both),
        check_vma=False,
    )
```
